256 devices in a mesh: dp: 64 (over x, z_hi, y), mp: 4 (over z_lo, core).
Axes of the slice: x: 4, y: 4, z: 8 (z_hi: 4, z_lo: 2; z = z_hi * 2 + z_lo), core: 2. Of those that a mesh axis runs over, the one named last changes fastest.
Arguments:
- history_sequences: float32 [512, 512], P('dp'), may hold values from -65 to 65, as said below
- later_steps: float32 [512, 128], P('dp'), may hold values from -65 to 65
- patch_lift_matrix: bfloat16 [32, 1280], P(None, 'dp'), may hold values from -1 to 1
- scaling_factors: bfloat16 [2, 1280], P(None, 'dp'), may hold values from 0.5 to 1.5
- asking_matrix: bfloat16 [1280, 1280], P('dp', 'mp'), may hold values from -0.15625 to 0.15625
- lookup_matrix: bfloat16 [1280, 1280], P('dp', 'mp'), may hold values from -0.15625 to 0.15625
- content_matrix: bfloat16 [1280, 1280], P('dp', 'mp'), may hold values from -0.15625 to 0.15625
- attend_exit_matrix: bfloat16 [1280, 1280], P('mp', 'dp'), may hold values from -0.15625 to 0.15625
- outlook_matrix: bfloat16 [1280, 1280], P('dp', 'mp'), may hold values from -0.15625 to 0.15625
Outputs:
- loss_mean: float32 [], replicated
- embed_grad: float32 [32, 1280], P(None, 'dp')
- gains_grad: float32 [2, 1280], P(None, 'dp')
- query_grad: float32 [1280, 1280], P('dp', 'mp')
- key_grad: float32 [1280, 1280], P('dp', 'mp')
- value_grad: float32 [1280, 1280], P('dp', 'mp')
- output_grad: float32 [1280, 1280], P('mp', 'dp')
- head_weight_gradient: float32 [1280, 1280], P('dp', 'mp')
The draws below stay inside these ranges and needn't reach their ends.
Inputs may be any that keep to these rules, and one draw needn't show every extreme that they name: `history_sequences`: later_steps continues the history of each series.
All inputs are finite; a program needn't handle non-finite values.
Results may differ from the reference program's by a relative error of at most 0.005.
Values may be sent and summed in bfloat16 or wider, within the bound.
No kernel may reach another device: no remote copies, remote signals or barrier semaphores. Data moves between devices by JAX's collectives and lax.ppermute only.
A program may use at most 64 MiB of HBM per device.

```python
import math
import jax
import jax.numpy as jnp
from jax import lax

MODEL_WIDTH = 1280
PATCH = 32
HORIZON_SPAN = 128
PATCHES = 16
LEVEL_CHANNELS = 10
HEAD_DIM = 80
PREDICT_COLUMNS = 1280
SERIES = 512
TOKENS = 8192


def history(key):
    total = PATCHES * PATCH + HORIZON_SPAN
    base = jax.random.fold_in(key, 7)
    parts = jax.random.split(base, 5)
    offset_level = 5.0 * jax.random.truncated_normal(parts[0], -3.0, 3.0, (SERIES, 1), dtype=jnp.float32)
    scale = jnp.exp(jax.random.uniform(parts[1], (SERIES, 1), minval=jnp.log(0.3), maxval=jnp.log(10.0)))
    noise = jax.random.truncated_normal(parts[2], -4.0, 4.0, (SERIES, total), dtype=jnp.float32)
    period = jax.random.uniform(parts[3], (SERIES, 1), minval=8.0, maxval=96.0)
    phase = jax.random.uniform(parts[4], (SERIES, 1), minval=0.0, maxval=2.0 * jnp.pi)
    steps = jnp.arange(total, dtype=jnp.float32)[None, :]
    wave = jnp.sin(2.0 * jnp.pi * steps / period + phase)
    return (offset_level + scale * (noise + wave)).astype(jnp.float32)


def draw_history_sequences(key, part):
    return history(key)[:, :PATCHES * PATCH]


def draw_later_steps(key, part):
    return history(key)[:, PATCHES * PATCH:]


def block_levels(key, dims, cuts, least, largest):
    def one(axis_at, blocks):
        steps = jax.random.uniform(jax.random.fold_in(jax.random.fold_in(key, 6), axis_at), (blocks,), jnp.float32, least / len(cuts), largest / len(cuts))
        return jnp.repeat(jnp.exp(steps), dims[axis_at] // blocks).reshape((-1,) + (1,) * (len(dims) - axis_at - 1))

    loudness = one(*cuts[0])
    for cut in cuts[1:]:
        loudness = loudness * one(*cut)
    return loudness


def bell_draw(key, dims, deviation, most, cuts=(), kind=jnp.bfloat16):
    drawn = jax.random.normal(key, dims, jnp.float32) * deviation
    if len(cuts) > 0:
        drawn = block_levels(key, dims, cuts, -0.22, 0.18) * drawn
    return jnp.clip(drawn, min=-most, max=most).astype(kind)


def setup_inputs(seed: int = 0) -> dict:
    seeds = jax.random.split(jax.random.key(seed), 10)
    return {
        "history_sequences": draw_history_sequences(jax.random.fold_in(seeds[9], 71), 0),
        "later_steps": draw_later_steps(jax.random.fold_in(seeds[9], 71), 0),
        "patch_lift_matrix": bell_draw(seeds[2], (PATCH, MODEL_WIDTH), PATCH ** -0.5, 1.0, ((1, 64),)),
        "scaling_factors": jnp.clip(1.0 + 0.1 * jax.random.normal(seeds[3], (2, MODEL_WIDTH), jnp.float32), 0.5, 1.5).astype(jnp.bfloat16),
        "asking_matrix": bell_draw(seeds[4], (MODEL_WIDTH, MODEL_WIDTH), MODEL_WIDTH ** -0.5, 0.15625, ((0, 64), (1, 4))),
        "lookup_matrix": bell_draw(seeds[5], (MODEL_WIDTH, MODEL_WIDTH), MODEL_WIDTH ** -0.5, 0.15625, ((0, 64), (1, 4))),
        "content_matrix": bell_draw(seeds[6], (MODEL_WIDTH, MODEL_WIDTH), MODEL_WIDTH ** -0.5, 0.15625, ((0, 64), (1, 4))),
        "attend_exit_matrix": bell_draw(seeds[7], (MODEL_WIDTH, MODEL_WIDTH), MODEL_WIDTH ** -0.5, 0.15625, ((0, 4), (1, 64))),
        "outlook_matrix": bell_draw(seeds[8], (MODEL_WIDTH, PREDICT_COLUMNS), MODEL_WIDTH ** -0.5, 0.15625, ((0, 64), (1, 4))),
    }


EPS = 1e-06
STAT_EPS = 1e-05
SMOOTHING_RADIUS = 0.05

def rms_forward(residual, gain):
    factor = lax.rsqrt(lax.optimization_barrier(jnp.mean(residual * residual, axis=1, keepdims=True)) + EPS)
    return ((residual * factor * gain[None, :]).astype(jnp.bfloat16), factor)

def rms_backward(residual, factor, gain, upstream):
    weighted = gain[None, :] * upstream
    inner = lax.optimization_barrier(jnp.mean(weighted * residual, axis=1, keepdims=True))
    back = factor * weighted - residual * factor * factor * factor * inner
    gain_term = lax.optimization_barrier(jnp.sum(upstream * residual * factor, axis=0))
    return (back, gain_term)

def positions(length, width):
    half = width // 2
    freqs = jnp.exp(-math.log(10000.0) * jnp.arange(half, dtype=jnp.float32) / half)
    angles = jnp.arange(length, dtype=jnp.float32)[:, None] * freqs[None, :]
    return jnp.concatenate([jnp.sin(angles), jnp.cos(angles)], axis=1)

def prepare(history_sequences, later_steps):
    number = history_sequences.shape[0]
    centre = lax.optimization_barrier(jnp.mean(history_sequences, axis=1, keepdims=True))
    spread = jnp.sqrt(lax.optimization_barrier(jnp.mean((history_sequences - centre) * (history_sequences - centre), axis=1, keepdims=True)) + STAT_EPS)
    normed = (history_sequences - centre) / spread
    ahead = (later_steps - centre) / spread
    joined = jnp.concatenate([normed, ahead], axis=1).reshape(number, -1, PATCH)
    reach = later_steps.shape[1] // PATCH
    future_values = jnp.concatenate([joined[:, offset + 1:offset + 1 + PATCHES] for offset in range(reach)], axis=2)
    future_values = future_values.reshape(number * PATCHES, reach * PATCH)
    patches = normed.reshape(number * PATCHES, PATCH).astype(jnp.bfloat16)
    return (patches, future_values)

def attention_forward(queries, keys, values, number):
    layout = (number, PATCHES, -1, HEAD_DIM)
    query_blocks = queries.reshape(layout).astype(jnp.float32)
    key_blocks = keys.reshape(layout).astype(jnp.float32)
    value_blocks = values.reshape(layout).astype(jnp.float32)
    scale = 1.0 / math.sqrt(HEAD_DIM)
    scores = jnp.einsum('sihd,sjhd->shij', query_blocks, key_blocks) * scale
    place = jnp.arange(PATCHES)
    causal = place[:, None] >= place[None, :]
    raised = jnp.where(causal, jnp.exp(scores), 0.0)
    probs = raised / lax.optimization_barrier(jnp.sum(raised, axis=3, keepdims=True))
    probs_low = probs.astype(jnp.bfloat16)
    context = jnp.einsum('shij,sjhd->sihd', probs_low.astype(jnp.float32), value_blocks)
    context = context.astype(jnp.bfloat16).reshape(number * PATCHES, -1)
    return (context, probs, probs_low)

def attention_backward(context_grad, queries, keys, values, probs, probs_low, number):
    layout = (number, PATCHES, -1, HEAD_DIM)
    query_blocks = queries.reshape(layout).astype(jnp.float32)
    key_blocks = keys.reshape(layout).astype(jnp.float32)
    value_blocks = values.reshape(layout).astype(jnp.float32)
    grad_blocks = context_grad.reshape(layout).astype(jnp.float32)
    scale = 1.0 / math.sqrt(HEAD_DIM)
    prob_grad = jnp.einsum('sihd,sjhd->shij', grad_blocks, value_blocks)
    value_back = jnp.einsum('shij,sihd->sjhd', probs_low.astype(jnp.float32), grad_blocks).astype(jnp.bfloat16)
    centred = prob_grad - lax.optimization_barrier(jnp.sum(probs * prob_grad, axis=3, keepdims=True))
    score_grad = (probs * centred * scale).astype(jnp.bfloat16).astype(jnp.float32)
    query_back = jnp.einsum('shij,sjhd->sihd', score_grad, key_blocks).astype(jnp.bfloat16)
    key_back = jnp.einsum('shij,sihd->sjhd', score_grad, query_blocks).astype(jnp.bfloat16)
    flat = (number * PATCHES, -1)
    return (query_back.reshape(flat), key_back.reshape(flat), value_back.reshape(flat))

def pinball_terms(estimate_entries, actual_entries):
    batch_example_tally = estimate_entries.shape[0]
    horizon_error = actual_entries[:, :, None] - estimate_entries.reshape(batch_example_tally, -1, LEVEL_CHANNELS)
    cumulative_share = jnp.arange(LEVEL_CHANNELS, dtype=jnp.float32) / LEVEL_CHANNELS
    mean_indicator = jnp.arange(LEVEL_CHANNELS) == 0
    lopsided_errors = jnp.where(mean_indicator, horizon_error * horizon_error, cumulative_share * horizon_error + SMOOTHING_RADIUS * jax.nn.softplus(-horizon_error / SMOOTHING_RADIUS))
    skew_coefficient = jnp.where(mean_indicator, -2.0 * horizon_error, jax.nn.sigmoid(-horizon_error / SMOOTHING_RADIUS) - cumulative_share) / HORIZON_SPAN
    return (jnp.sum(lopsided_errors) / HORIZON_SPAN, skew_coefficient.reshape(batch_example_tally, -1).astype(jnp.bfloat16))

def reference(history_sequences, later_steps, patch_lift_matrix, scaling_factors, asking_matrix, lookup_matrix, content_matrix, attend_exit_matrix, outlook_matrix):
    number = history_sequences.shape[0]
    patches, future_values = prepare(history_sequences, later_steps)
    gains = scaling_factors.astype(jnp.float32)
    residual_zero = jnp.dot(patches, patch_lift_matrix, preferred_element_type=jnp.float32) + jnp.tile(positions(PATCHES, MODEL_WIDTH), (number, 1))
    normed_attn, factor_attn = rms_forward(residual_zero, gains[0])
    queries = jnp.dot(normed_attn, asking_matrix, preferred_element_type=jnp.float32).astype(jnp.bfloat16)
    keys = jnp.dot(normed_attn, lookup_matrix, preferred_element_type=jnp.float32).astype(jnp.bfloat16)
    values = jnp.dot(normed_attn, content_matrix, preferred_element_type=jnp.float32).astype(jnp.bfloat16)
    context, probs, probs_low = attention_forward(queries, keys, values, number)
    residual_one = residual_zero + jnp.dot(context, attend_exit_matrix, preferred_element_type=jnp.float32)
    normed_head, factor_head = rms_forward(residual_one, gains[1])
    estimate_entries = jnp.dot(normed_head, outlook_matrix, preferred_element_type=jnp.float32)
    total_loss_value, estimate_derivative = pinball_terms(estimate_entries, future_values)
    loss_mean = total_loss_value / TOKENS
    head_weight_gradient = jnp.dot(normed_head.T, estimate_derivative, preferred_element_type=jnp.float32)
    head_reverse = jnp.dot(estimate_derivative, outlook_matrix.T, preferred_element_type=jnp.float32)
    residual_one_grad, gain_one = rms_backward(residual_one, factor_head, gains[1], head_reverse)
    attn_low = residual_one_grad.astype(jnp.bfloat16)
    output_grad = jnp.dot(context.T, attn_low, preferred_element_type=jnp.float32)
    context_grad = jnp.dot(attn_low, attend_exit_matrix.T, preferred_element_type=jnp.float32).astype(jnp.bfloat16)
    query_back, key_back, value_back = attention_backward(context_grad, queries, keys, values, probs, probs_low, number)
    query_grad = jnp.dot(normed_attn.T, query_back, preferred_element_type=jnp.float32)
    key_grad = jnp.dot(normed_attn.T, key_back, preferred_element_type=jnp.float32)
    value_grad = jnp.dot(normed_attn.T, value_back, preferred_element_type=jnp.float32)
    attn_back = jnp.dot(query_back, asking_matrix.T, preferred_element_type=jnp.float32)
    attn_back = attn_back + jnp.dot(key_back, lookup_matrix.T, preferred_element_type=jnp.float32)
    attn_back = attn_back + jnp.dot(value_back, content_matrix.T, preferred_element_type=jnp.float32)
    norm_back_zero, gain_zero = rms_backward(residual_zero, factor_attn, gains[0], attn_back)
    residual_zero_grad = residual_one_grad + norm_back_zero
    embed_grad = jnp.dot(patches.T, residual_zero_grad.astype(jnp.bfloat16), preferred_element_type=jnp.float32)
    gains_grad = jnp.stack([gain_zero, gain_one], axis=0)
    return (loss_mean, embed_grad, gains_grad, query_grad, key_grad, value_grad, output_grad, head_weight_gradient)
```

```python
import math

import jax
import jax.numpy as jnp
import numpy as np
from jax import lax
from jax.experimental import pallas as pl
from jax.experimental.pallas import tpu as pltpu
from jax.sharding import Mesh
from jax.sharding import PartitionSpec as P

WIDTH = 1280
PATCH = 32
PATCHES = 16
HEAD_DIM = 80
CHANNELS = 10
BLOCKS = 64
OWN = WIDTH // BLOCKS
PADDED = 24
ROWS = BLOCKS * PADDED
TOKENS = 128
COLS = 320
WIDE = 384
BASIS = PATCH + PATCHES
TILES = (BASIS // 8) * (3 * WIDE // 128)
DP = ("dp_0", "dp_1", "dp_2")
MP = ("mp_0", "mp_1")
EPS = 1e-06
STAT_EPS = 1e-05
RADIUS = 0.05
SCALE = 1.0 / math.sqrt(HEAD_DIM)
BF = jnp.bfloat16
F32 = jnp.float32


def nn(a, b):
    return lax.dot_general(a, b, (((1,), (0,)), ((), ())), preferred_element_type=F32)


def nt(a, b):
    return lax.dot_general(a, b, (((1,), (1,)), ((), ())), preferred_element_type=F32)


def tn(a, b):
    return lax.dot_general(a, b, (((0,), (0,)), ((), ())), preferred_element_type=F32)


def two(x):
    high = x.astype(BF)
    return high, (x - high.astype(F32)).astype(BF)


def position_table():
    half = WIDTH // 2
    freqs = np.exp(np.float32(-math.log(10000.0)) * np.arange(half, dtype=np.float32) / np.float32(half))
    angles = np.arange(PATCHES, dtype=np.float32)[:, None] * freqs[None, :]
    table = np.concatenate([np.sin(angles), np.cos(angles)], axis=1).astype(np.float32)
    return np.ascontiguousarray(table.reshape(PATCHES, BLOCKS, OWN).transpose(1, 0, 2))


def call(body, outs, *args):
    return pl.pallas_call(
        body,
        out_shape=[jax.ShapeDtypeStruct(s, d) for s, d in outs],
        name=body.__name__,
    )(*args)


def basis_kernel(embed_ref, gains_ref, pos_ref, wq_ref, wk_ref, wv_ref, out_ref):
    basis = jnp.concatenate([embed_ref[...].astype(F32), pos_ref[...]], axis=0)
    high, low = two(basis * gains_ref[0:1, :].astype(F32))
    out_ref[...] = jnp.zeros_like(out_ref)
    for w, ref in enumerate((wq_ref, wk_ref, wv_ref)):
        weight = ref[...]
        part = nn(high, weight) + nn(low, weight)
        for i in range(BASIS // 8):
            rows = part[8 * i : 8 * i + 8]
            out_ref[9 * i + 3 * w] = rows[:, 0:128]
            out_ref[9 * i + 3 * w + 1] = rows[:, 128:256]
            out_ref[9 * i + 3 * w + 2, :, 0:64] = rows[:, 256:320]


def from_tiles(ref):
    return jnp.concatenate(
        [jnp.concatenate([ref[9 * i + j] for j in range(9)], axis=1) for i in range(BASIS // 8)], axis=0
    )


def raw_projections(tiles_ref, basis):
    high, low = two(from_tiles(tiles_ref))
    return tn(jnp.concatenate([high, low], axis=0), jnp.concatenate([basis, basis], axis=0))


def first_residual(exit_ref, basis_ref):
    lanes = exit_ref[:, 256:384]
    entries = basis_ref[...]
    return nn(lanes, jnp.concatenate([jnp.zeros_like(entries), entries], axis=0))


def causal_mask():
    j = lax.broadcasted_iota(jnp.int32, (TOKENS, TOKENS), 0)
    i = lax.broadcasted_iota(jnp.int32, (TOKENS, TOKENS), 1)
    same = lax.shift_right_logical(j, 4) == lax.shift_right_logical(i, 4)
    return same & (j <= i)


def attention_kernel(
    exit_ref, tiles_ref, basis_ref, part_ref, context_ref, queries_ref, keys_ref, values_ref, probs_ref, factor_ref
):
    residual = first_residual(exit_ref, basis_ref)
    factor = lax.rsqrt(jnp.sum(residual * residual, axis=0, keepdims=True) / WIDTH + EPS)
    factor_ref[...] = jnp.broadcast_to(factor, factor_ref.shape)
    raw = raw_projections(tiles_ref, basis_ref[0:BASIS, :]) * factor
    queries_ref[...] = raw[0:COLS].astype(BF)
    keys_ref[...] = raw[WIDE : WIDE + COLS].astype(BF)
    values_ref[...] = raw[2 * WIDE : 2 * WIDE + COLS].astype(BF)
    mask = causal_mask()
    for h in range(COLS // HEAD_DIM):
        at = slice(h * HEAD_DIM, (h + 1) * HEAD_DIM)
        scores = tn(keys_ref[at, :], queries_ref[at, :]) * SCALE
        raised = jnp.where(mask, jnp.exp(scores), 0.0)
        probs = raised / jnp.sum(raised, axis=0, keepdims=True)
        probs_ref[h] = probs
        context_ref[at, :] = nn(values_ref[at, :], probs.astype(BF)).astype(BF)
    part_ref[...] = nn(exit_ref[:, 0:COLS], context_ref[...]).astype(BF)


def head_kernel(
    exit_ref, head_ref, basis_ref, near_ref, far_ref, target_ref, back_ref, grad_ref, residual_ref, factor_ref, loss_ref
):
    residual = first_residual(exit_ref, basis_ref) + (near_ref[...].astype(F32) + far_ref[...].astype(F32))
    residual_ref[...] = residual
    factor = lax.rsqrt(jnp.sum(residual * residual, axis=0, keepdims=True) / WIDTH + EPS)
    factor_ref[...] = jnp.broadcast_to(factor, factor_ref.shape)
    scaled = residual * factor
    normed = (scaled * head_ref[:, COLS + 1 : COLS + 2].astype(F32)).astype(BF)
    forecast = tn(head_ref[...], normed)[0:COLS]
    column = lax.broadcasted_iota(jnp.int32, (COLS, 1), 0).astype(F32)
    step = jnp.floor((column + 0.5) * 0.1)
    channel = column - CHANNELS * step
    spread = (step == lax.broadcasted_iota(jnp.int32, (COLS, PATCH), 1).astype(F32)).astype(F32).astype(BF)
    target = target_ref[...]
    first, rest = target.astype(BF), target
    rest = rest - first.astype(F32)
    second, third = two(rest)
    expanded = nn(spread, first) + (nn(spread, second) + nn(spread, third))
    error = expanded - forecast
    share = channel / CHANNELS
    mean_channel = channel == 0.0
    inside = error / -RADIUS
    tail = jnp.exp(-jnp.abs(inside))
    softplus = jnp.maximum(inside, 0.0) + jnp.log1p(tail)
    sigmoid = jnp.where(inside >= 0.0, 1.0, tail) / (1.0 + tail)
    terms = jnp.where(mean_channel, error * error, share * error + RADIUS * softplus)
    loss_ref[...] = jnp.broadcast_to(jnp.sum(terms, axis=0, keepdims=True), loss_ref.shape)
    slope = (jnp.where(mean_channel, -2.0 * error, sigmoid - share) * (1.0 / 128.0)).astype(BF)
    slope = jnp.concatenate([slope, jnp.zeros((WIDE - COLS, TOKENS), BF)], axis=0)
    back = nn(head_ref[...], slope)
    back_ref[...] = back.astype(BF)
    high, low = two(jnp.sum(back * scaled, axis=1, keepdims=True))
    lane = lax.broadcasted_iota(jnp.int32, (1, WIDE), 1)
    grad = nt(normed, slope)
    grad = jnp.where(lane == COLS, high.astype(F32), jnp.where(lane == COLS + 1, low.astype(F32), grad))
    grad_ref[...] = grad.astype(BF)


def backward_kernel(
    exit_ref,
    head_ref,
    tiles_ref,
    basis_ref,
    near_ref,
    far_ref,
    residual_ref,
    factor_one_ref,
    factor_zero_ref,
    context_ref,
    queries_ref,
    keys_ref,
    values_ref,
    probs_ref,
    loss_ref,
    grad_ref,
    out_ref,
):
    basis = basis_ref[0:BASIS, :]
    patches = basis_ref[0:PATCH, :]
    upstream = near_ref[...].astype(F32) + far_ref[...].astype(F32)
    residual = residual_ref[...]
    factor = factor_one_ref[0:1, :]
    weighted = head_ref[:, COLS + 1 : COLS + 2].astype(F32) * upstream
    inner = jnp.sum(weighted * residual, axis=0, keepdims=True) / WIDTH
    low = (factor * weighted - residual * (factor * factor * factor * inner)).astype(BF)
    grad = nt(low, jnp.concatenate([context_ref[...], patches, patches], axis=0))
    lane = lax.broadcasted_iota(jnp.int32, (1, WIDE), 1)
    grad = jnp.where(lane >= COLS + PATCH, grad - grad.astype(BF).astype(F32), grad)
    grad_ref[...] = grad.astype(BF)
    context_grad = tn(exit_ref[...], low)[0:COLS].astype(BF)
    backs = ([], [], [])
    for h in range(COLS // HEAD_DIM):
        at = slice(h * HEAD_DIM, (h + 1) * HEAD_DIM)
        slope = context_grad[at]
        probs = probs_ref[h]
        prob_grad = tn(values_ref[at, :], slope)
        value_back = nt(slope, probs.astype(BF))
        centred = prob_grad - jnp.sum(probs * prob_grad, axis=0, keepdims=True)
        score_grad = (probs * centred * SCALE).astype(BF)
        backs[0].append(nn(keys_ref[at, :], score_grad).astype(BF))
        backs[1].append(nt(queries_ref[at, :], score_grad).astype(BF))
        backs[2].append(value_back.astype(BF))
    gap = jnp.zeros((WIDE - COLS, TOKENS), BF)
    back = jnp.concatenate([*backs[0], gap, *backs[1], gap, *backs[2], gap], axis=0)
    factor = factor_zero_ref[0:1, :]
    entries = basis.astype(F32)
    high, low = two(entries * factor)
    total = nt(high, back) + nt(low, back)
    raw = raw_projections(tiles_ref, basis)
    inner = jnp.sum(back.astype(F32) * raw, axis=0, keepdims=True) / WIDTH
    high, low = two(entries * (factor * factor * factor * inner))
    mixed = nt(high, patches) + nt(low, patches)
    out_ref[...] = jnp.zeros_like(out_ref)
    for i in range(BASIS // 8):
        for j in range(9):
            out_ref[9 * i + j] = total[8 * i : 8 * i + 8, 128 * j : 128 * j + 128]
        out_ref[TILES + i, :, 0:PATCH] = mixed[8 * i : 8 * i + 8]
    out_ref[TILES + BASIS // 8] = loss_ref[...]


def exact(dims):
    def dot(a, b):
        return lax.dot_general(a, b, (dims, ((), ())), precision=lax.Precision.HIGHEST, preferred_element_type=F32)

    return dot


def last_kernel(
    tiles_ref, embed_ref, gains_ref, pos_ref, wq_ref, wk_ref, wv_ref, exit_ref, head_ref, q_ref, k_ref, v_ref, rest_ref
):
    basis = jnp.concatenate([embed_ref[...].astype(F32), pos_ref[...]], axis=0)
    scaled = basis * gains_ref[0:1, :].astype(F32)
    total = from_tiles(tiles_ref)
    scaled_grad = exact(((0,), (0,)))(scaled, total)
    plain_grad = exact(((0,), (0,)))(basis, total)
    embed = jnp.zeros((OWN, PATCH), F32)
    gain_zero = jnp.zeros((OWN, 1), F32)
    for w, (weight_ref, out_ref) in enumerate(((wq_ref, q_ref), (wk_ref, k_ref), (wv_ref, v_ref))):
        weight = weight_ref[...].astype(F32)
        out_ref[...] = scaled_grad[:, w * WIDE : w * WIDE + COLS]
        gain_zero += jnp.sum(weight * plain_grad[:, w * WIDE : w * WIDE + COLS], axis=1, keepdims=True)
        embed += exact(((1,), (1,)))(weight, total[0:PATCH, w * WIDE : w * WIDE + COLS])
    pick = (lax.broadcasted_iota(jnp.int32, (2, PATCH), 0) == 0).astype(F32)
    embed = embed * exact(((0,), (0,)))(gains_ref[...].astype(F32), pick)
    mixed = jnp.concatenate([tiles_ref[TILES + i] for i in range(BASIS // 8)], axis=0)[:, 0:PATCH]
    embed = embed - exact(((0,), (0,)))(basis, mixed)
    ends = exit_ref[0:OWN, COLS : COLS + PATCH] + exit_ref[0:OWN, COLS + PATCH : WIDE]
    gain_one = head_ref[0:OWN, COLS : COLS + 1] + head_ref[0:OWN, COLS + 1 : COLS + 2]
    loss = jnp.sum(tiles_ref[TILES + BASIS // 8][0:1, :], axis=1, keepdims=True)
    rest_ref[...] = jnp.zeros_like(rest_ref)
    rest_ref[0:OWN, 0:PATCH] = embed + 0.25 * ends
    rest_ref[0:OWN, PATCH : PATCH + 1] = gain_zero
    rest_ref[0:OWN, PATCH + 1 : PATCH + 2] = gain_one
    rest_ref[0:1, PATCH + 2 : PATCH + 3] = loss


def swapped(x, axis):
    return lax.ppermute(x, axis, [(0, 1), (1, 0)])


def mp_parts(part):
    near = (part.astype(F32) + swapped(part, "mp_1").astype(F32)).astype(BF)
    return near, swapped(near, "mp_0")


def to_everyone(x):
    return lax.all_to_all(jnp.broadcast_to(x[None], (BLOCKS, *x.shape)), DP, 0, 0, tiled=True)


def summed(x):
    return jnp.sum(lax.all_to_all(x, DP, 0, 0, tiled=True).astype(F32), axis=0)


def padded_rows(x):
    return jnp.pad(x, ((0, PADDED - OWN), (0, WIDE - x.shape[1])))


def prepare(history, later):
    number = history.shape[0]
    centre = jnp.mean(history, axis=1, keepdims=True)
    spread = jnp.sqrt(jnp.mean((history - centre) * (history - centre), axis=1, keepdims=True) + STAT_EPS)
    normed = (history - centre) / spread
    ahead = (later - centre) / spread
    joined = jnp.concatenate([normed, ahead], axis=1).reshape(number, -1, PATCH)
    member = lax.axis_index(MP)
    target = lax.dynamic_slice_in_dim(joined, member + 1, PATCHES, 1).reshape(number * PATCHES, PATCH)
    patches = joined[:, :PATCHES].reshape(number * PATCHES, PATCH).astype(BF)
    return patches.T, target.T


def per_device(history, later, embed, gains, asking, lookup, content, attend_exit, outlook):
    place = lax.axis_index(DP)
    pos = lax.dynamic_index_in_dim(jnp.asarray(position_table()), place, 0, keepdims=False)
    pos_high, pos_low = two(pos)
    exit_block = padded_rows(jnp.concatenate([attend_exit.T, embed.T, pos_high.T, pos_low.T], axis=1))
    head_block = padded_rows(jnp.concatenate([outlook, gains.T], axis=1))

    tiles = call(basis_kernel, [((BLOCKS, 8, 128), F32)], embed, gains, pos, asking, lookup, content)[0]
    tiles = to_everyone(summed(tiles))
    exit_all = to_everyone(exit_block).reshape(ROWS, WIDE)
    head_all = to_everyone(head_block).reshape(ROWS, WIDE)

    patches, target = prepare(history, later)
    number = np.arange(TOKENS) % PATCHES
    place_hot = jnp.asarray((np.arange(PATCHES)[:, None] == number[None, :]), dtype=BF)
    basis = jnp.concatenate([patches, place_hot, place_hot], axis=0)

    turned = (COLS, TOKENS)
    part, context, queries, keys, values, probs, factor_zero = call(
        attention_kernel,
        [
            ((ROWS, TOKENS), BF),
            (turned, BF),
            (turned, BF),
            (turned, BF),
            (turned, BF),
            ((COLS // HEAD_DIM, TOKENS, TOKENS), F32),
            ((8, TOKENS), F32),
        ],
        exit_all,
        tiles,
        basis,
    )
    near, far = mp_parts(part)
    back, head_grad, residual, factor_one, loss = call(
        head_kernel,
        [
            ((ROWS, TOKENS), BF),
            ((ROWS, WIDE), BF),
            ((ROWS, TOKENS), F32),
            ((8, TOKENS), F32),
            ((8, TOKENS), F32),
        ],
        exit_all,
        head_all,
        basis,
        near,
        far,
        target,
    )
    near, far = mp_parts(back)
    exit_grad, totals = call(
        backward_kernel,
        [((ROWS, WIDE), BF), ((BLOCKS, 8, 128), F32)],
        exit_all,
        head_all,
        tiles,
        basis,
        near,
        far,
        residual,
        factor_one,
        factor_zero,
        context,
        queries,
        keys,
        values,
        probs,
        loss,
    )
    totals = to_everyone(summed(totals))
    head_sum = summed(head_grad.reshape(BLOCKS, PADDED, WIDE))
    exit_sum = summed(exit_grad.reshape(BLOCKS, PADDED, WIDE))
    own = (OWN, COLS)
    query_grad, key_grad, value_grad, rest = call(
        last_kernel,
        [(own, F32), (own, F32), (own, F32), ((PADDED, 128), F32)],
        totals,
        embed,
        gains,
        pos,
        asking,
        lookup,
        content,
        exit_sum,
        head_sum,
    )
    rest = rest + swapped(rest, "mp_1")
    rest = rest + swapped(rest, "mp_0")
    loss_mean = rest[0, PATCH + 2] / 1048576.0
    return (
        loss_mean,
        rest[:OWN, :PATCH].T,
        rest[:OWN, PATCH : PATCH + 2].T,
        query_grad,
        key_grad,
        value_grad,
        exit_sum[:OWN, :COLS].T,
        head_sum[:OWN, :COLS],
    )


def solution(mesh):
    split = Mesh(mesh.devices.reshape(4, 4, 4, 2, 2), ("dp_0", "dp_1", "dp_2", "mp_0", "mp_1"))
    placed = (
        P(DP, None),
        P(DP, None),
        P(None, DP),
        P(None, DP),
        P(DP, MP),
        P(DP, MP),
        P(DP, MP),
        P(MP, DP),
        P(DP, MP),
    )
    return jax.shard_map(
        per_device,
        mesh=split,
        in_specs=placed,
        out_specs=(
            P(),
            P(None, DP),
            P(None, DP),
            P(DP, MP),
            P(DP, MP),
            P(DP, MP),
            P(MP, DP),
            P(DP, MP),
        ),
        check_vma=False,
    )
```

```python
import math

import jax
import jax.numpy as jnp
import numpy as np
from jax import lax
from jax.experimental import pallas as pl
from jax.experimental.pallas import tpu as pltpu
from jax.sharding import Mesh
from jax.sharding import PartitionSpec as P

WIDTH = 1280
PATCH = 32
PATCHES = 16
HEAD_DIM = 80
CHANNELS = 10
BLOCKS = 64
OWN = WIDTH // BLOCKS
PADDED = 24
ROWS = BLOCKS * PADDED
TOKENS = 128
COLS = 320
WIDE = 384
BASIS = PATCH + PATCHES
TILES = (BASIS // 8) * (3 * WIDE // 128)
DP = ("dp_0", "dp_1", "dp_2")
XY = ("dp_0", "dp_2")
Z = "dp_1"
GROUPS = 16
DEPTH = 4
GROUP_ROWS = DEPTH * PADDED
SMALL = 8 * BLOCKS // GROUPS
HALF = ROWS // 2
MP = ("mp_0", "mp_1")
EPS = 1e-06
STAT_EPS = 1e-05
RADIUS = 0.05
SCALE = 1.0 / math.sqrt(HEAD_DIM)
BF = jnp.bfloat16
F32 = jnp.float32


def nn(a, b):
    return lax.dot_general(a, b, (((1,), (0,)), ((), ())), preferred_element_type=F32)


def nt(a, b):
    return lax.dot_general(a, b, (((1,), (1,)), ((), ())), preferred_element_type=F32)


def tn(a, b):
    return lax.dot_general(a, b, (((0,), (0,)), ((), ())), preferred_element_type=F32)


def two(x):
    high = x.astype(BF)
    return high, (x - high.astype(F32)).astype(BF)


def position_table():
    half = WIDTH // 2
    freqs = np.exp(np.float32(-math.log(10000.0)) * np.arange(half, dtype=np.float32) / np.float32(half))
    angles = np.arange(PATCHES, dtype=np.float32)[:, None] * freqs[None, :]
    table = np.concatenate([np.sin(angles), np.cos(angles)], axis=1).astype(np.float32)
    return np.ascontiguousarray(table.reshape(PATCHES, BLOCKS, OWN).transpose(1, 0, 2))


def call(body, outs, *args):
    return pl.pallas_call(
        body,
        out_shape=[jax.ShapeDtypeStruct(s, d) for s, d in outs],
        name=body.__name__,
    )(*args)


def basis_kernel(embed_ref, gains_ref, pos_ref, wq_ref, wk_ref, wv_ref, out_ref):
    basis = jnp.concatenate([embed_ref[...].astype(F32), pos_ref[...]], axis=0)
    high, low = two(basis * gains_ref[0:1, :].astype(F32))
    out_ref[...] = jnp.zeros_like(out_ref)
    for w, ref in enumerate((wq_ref, wk_ref, wv_ref)):
        weight = ref[...]
        part = nn(high, weight) + nn(low, weight)
        for i in range(BASIS // 8):
            rows = part[8 * i : 8 * i + 8]
            out_ref[9 * i + 3 * w] = rows[:, 0:128]
            out_ref[9 * i + 3 * w + 1] = rows[:, 128:256]
            out_ref[9 * i + 3 * w + 2, :, 0:64] = rows[:, 256:320]


def from_tiles(ref):
    return jnp.concatenate(
        [jnp.concatenate([ref[9 * i + j] for j in range(9)], axis=1) for i in range(BASIS // 8)], axis=0
    )


def both_from(ref):
    def tile(t, lanes):
        return ref[t // DEPTH, GROUP_ROWS : GROUP_ROWS + SMALL, lanes].astype(F32)[8 * (t % DEPTH) : 8 * (t % DEPTH) + 8]

    return [
        jnp.concatenate(
            [jnp.concatenate([tile(9 * i + j, lanes) for j in range(9)], axis=1) for i in range(BASIS // 8)], axis=0
        ).astype(BF)
        for lanes in (slice(0, 128), slice(128, 256))
    ]


def blocks(ref, lanes=slice(0, WIDE)):
    rows = ref[:, 0:GROUP_ROWS, lanes]
    return rows.reshape(ROWS, rows.shape[2])


def spread_halves(value, mine_ref, other_ref):
    north = lax.axis_index("mp_1") == 1
    mine_ref[...] = jnp.where(north, value[HALF:], value[:HALF]).astype(BF)
    other_ref[...] = jnp.where(north, value[:HALF], value[HALF:]).astype(BF)


def joined_halves(mine_ref, other_ref):
    north = lax.axis_index("mp_1") == 1
    mine, other = mine_ref[...].astype(F32), other_ref[...].astype(F32)
    return jnp.concatenate([jnp.where(north, other, mine), jnp.where(north, mine, other)], axis=0)


def raw_projections(tiles_ref, basis):
    high, low = both_from(tiles_ref)
    return tn(jnp.concatenate([high, low], axis=0), jnp.concatenate([basis, basis], axis=0))


def first_residual(exit_ref, basis_ref):
    lanes = blocks(exit_ref, slice(256, 384))
    entries = basis_ref[...]
    return nn(lanes, jnp.concatenate([jnp.zeros_like(entries), entries], axis=0))


def causal_mask():
    j = lax.broadcasted_iota(jnp.int32, (TOKENS, TOKENS), 0)
    i = lax.broadcasted_iota(jnp.int32, (TOKENS, TOKENS), 1)
    same = lax.shift_right_logical(j, 4) == lax.shift_right_logical(i, 4)
    return same & (j <= i)


def attention_kernel(
    exit_ref, basis_ref, mine_ref, other_ref, context_ref, queries_ref, keys_ref, values_ref, probs_ref, factor_ref
):
    residual = first_residual(exit_ref, basis_ref)
    factor = lax.rsqrt(jnp.sum(residual * residual, axis=0, keepdims=True) / WIDTH + EPS)
    factor_ref[...] = jnp.broadcast_to(factor, factor_ref.shape)
    raw = raw_projections(exit_ref, basis_ref[0:BASIS, :]) * factor
    queries_ref[...] = raw[0:COLS].astype(BF)
    keys_ref[...] = raw[WIDE : WIDE + COLS].astype(BF)
    values_ref[...] = raw[2 * WIDE : 2 * WIDE + COLS].astype(BF)
    mask = causal_mask()
    for h in range(COLS // HEAD_DIM):
        at = slice(h * HEAD_DIM, (h + 1) * HEAD_DIM)
        scores = tn(keys_ref[at, :], queries_ref[at, :]) * SCALE
        raised = jnp.where(mask, jnp.exp(scores), 0.0)
        probs = raised / jnp.sum(raised, axis=0, keepdims=True)
        probs_ref[h] = probs
        context_ref[at, :] = nn(values_ref[at, :], probs.astype(BF)).astype(BF)
    context = jnp.concatenate([context_ref[...], jnp.zeros((WIDE - COLS, TOKENS), BF)], axis=0)
    spread_halves(nn(blocks(exit_ref), context), mine_ref, other_ref)


def head_kernel(
    exit_ref,
    head_ref,
    basis_ref,
    half_ref,
    rest_ref,
    target_ref,
    mine_ref,
    other_ref,
    grad_ref,
    residual_ref,
    factor_ref,
    loss_ref,
):
    head = blocks(head_ref)
    residual = first_residual(exit_ref, basis_ref) + joined_halves(half_ref, rest_ref)
    residual_ref[...] = residual
    factor = lax.rsqrt(jnp.sum(residual * residual, axis=0, keepdims=True) / WIDTH + EPS)
    factor_ref[...] = jnp.broadcast_to(factor, factor_ref.shape)
    scaled = residual * factor
    normed = (scaled * head[:, COLS + 1 : COLS + 2].astype(F32)).astype(BF)
    forecast = tn(head, normed)[0:COLS]
    column = lax.broadcasted_iota(jnp.int32, (COLS, 1), 0).astype(F32)
    step = jnp.floor((column + 0.5) * 0.1)
    channel = column - CHANNELS * step
    spread = (step == lax.broadcasted_iota(jnp.int32, (COLS, PATCH), 1).astype(F32)).astype(F32).astype(BF)
    target = target_ref[...]
    first, rest = target.astype(BF), target
    rest = rest - first.astype(F32)
    second, third = two(rest)
    expanded = nn(spread, first) + (nn(spread, second) + nn(spread, third))
    error = expanded - forecast
    share = channel / CHANNELS
    mean_channel = channel == 0.0
    inside = error / -RADIUS
    tail = jnp.exp(-jnp.abs(inside))
    softplus = jnp.maximum(inside, 0.0) + jnp.log1p(tail)
    sigmoid = jnp.where(inside >= 0.0, 1.0, tail) / (1.0 + tail)
    terms = jnp.where(mean_channel, error * error, share * error + RADIUS * softplus)
    loss_ref[...] = jnp.broadcast_to(jnp.sum(terms, axis=0, keepdims=True), loss_ref.shape)
    slope = (jnp.where(mean_channel, -2.0 * error, sigmoid - share) * (1.0 / 128.0)).astype(BF)
    slope = jnp.concatenate([slope, jnp.zeros((WIDE - COLS, TOKENS), BF)], axis=0)
    back = nn(head, slope)
    spread_halves(back, mine_ref, other_ref)
    high, low = two(jnp.sum(back * scaled, axis=1, keepdims=True))
    lane = lax.broadcasted_iota(jnp.int32, (1, WIDE), 1)
    grad = nt(normed, slope)
    grad = jnp.where(lane == COLS, high.astype(F32), jnp.where(lane == COLS + 1, low.astype(F32), grad))
    grad_ref[...] = grad.astype(BF).reshape(GROUPS, GROUP_ROWS, WIDE)


def backward_kernel(
    exit_ref,
    head_ref,
    basis_ref,
    half_ref,
    rest_ref,
    residual_ref,
    factor_one_ref,
    factor_zero_ref,
    context_ref,
    queries_ref,
    keys_ref,
    values_ref,
    probs_ref,
    loss_ref,
    out_ref,
):
    basis = basis_ref[0:BASIS, :]
    patches = basis_ref[0:PATCH, :]
    upstream = joined_halves(half_ref, rest_ref)
    residual = residual_ref[...]
    factor = factor_one_ref[0:1, :]
    weighted = blocks(head_ref, slice(256, 384))[:, COLS - 255 : COLS - 254].astype(F32) * upstream
    inner = jnp.sum(weighted * residual, axis=0, keepdims=True) / WIDTH
    low = (factor * weighted - residual * (factor * factor * factor * inner)).astype(BF)
    grad = nt(low, jnp.concatenate([context_ref[...], patches, patches], axis=0))
    lane = lax.broadcasted_iota(jnp.int32, (1, WIDE), 1)
    grad = jnp.where(lane >= COLS + PATCH, grad - grad.astype(BF).astype(F32), grad)
    out_ref[:, 0:GROUP_ROWS, :] = grad.astype(BF).reshape(GROUPS, GROUP_ROWS, WIDE)
    context_grad = tn(blocks(exit_ref), low)[0:COLS].astype(BF)
    backs = ([], [], [])
    for h in range(COLS // HEAD_DIM):
        at = slice(h * HEAD_DIM, (h + 1) * HEAD_DIM)
        slope = context_grad[at]
        probs = probs_ref[h]
        prob_grad = tn(values_ref[at, :], slope)
        value_back = nt(slope, probs.astype(BF))
        centred = prob_grad - jnp.sum(probs * prob_grad, axis=0, keepdims=True)
        score_grad = (probs * centred * SCALE).astype(BF)
        backs[0].append(nn(keys_ref[at, :], score_grad).astype(BF))
        backs[1].append(nt(queries_ref[at, :], score_grad).astype(BF))
        backs[2].append(value_back.astype(BF))
    gap = jnp.zeros((WIDE - COLS, TOKENS), BF)
    back = jnp.concatenate([*backs[0], gap, *backs[1], gap, *backs[2], gap], axis=0)
    factor = factor_zero_ref[0:1, :]
    entries = basis.astype(F32)
    high, low = two(entries * factor)
    total = nt(high, back) + nt(low, back)
    raw = raw_projections(exit_ref, basis)
    inner = jnp.sum(back.astype(F32) * raw, axis=0, keepdims=True) / WIDTH
    high, low = two(entries * (factor * factor * factor * inner))
    mixed = nt(high, patches) + nt(low, patches)
    blank = jnp.zeros((8, 128 - PATCH), F32)
    tiles = [total[8 * i : 8 * i + 8, 128 * j : 128 * j + 128] for i in range(BASIS // 8) for j in range(9)]
    tiles += [jnp.concatenate([mixed[8 * i : 8 * i + 8], blank], axis=1) for i in range(BASIS // 8)]
    tiles += [loss_ref[...]]
    tiles += [jnp.zeros((8, 128), F32)] * (BLOCKS - len(tiles))
    for k in range(GROUPS):
        high, low = two(jnp.concatenate(tiles[DEPTH * k : DEPTH * k + DEPTH], axis=0))
        out_ref[k, GROUP_ROWS : GROUP_ROWS + SMALL, :] = jnp.concatenate([high, low, jnp.zeros_like(low)], axis=1)


def pair(x):
    high, low = two(x)
    return jnp.concatenate([high, low, jnp.zeros_like(low)], axis=1)


def lined(block):
    return jnp.concatenate([block.astype(F32), jnp.zeros((SMALL - PADDED, WIDE), F32)], axis=0).astype(BF)


def blocks_out_kernel(tiles_ref, exit_ref, head_ref, out_ref):
    total = tiles_ref[0]
    for k in range(1, GROUPS):
        total += tiles_ref[k]
    block = jnp.concatenate([lined(exit_ref[...]), lined(head_ref[...]), pair(total)], axis=0)
    for z in range(DEPTH):
        out_ref[z] = block


def column_kernel(in_ref, exit_ref, head_ref):
    parts = [in_ref[z].astype(F32) for z in range(DEPTH)]
    total = sum(p[2 * SMALL :, 0:128] + p[2 * SMALL :, 128:256] for p in parts)
    exits = jnp.concatenate([p[0:PADDED] for p in parts], axis=0).astype(BF)
    heads = jnp.concatenate([p[SMALL : SMALL + PADDED] for p in parts], axis=0).astype(BF)
    exits = jnp.concatenate([exits, pair(total)], axis=0)
    for k in range(GROUPS):
        exit_ref[k] = exits
        head_ref[k] = heads


def scatter_kernel(head_ref, exit_ref, out_ref):
    heads = head_ref[0].astype(F32)
    exits = exit_ref[0].astype(F32)
    for k in range(1, GROUPS):
        heads += head_ref[k].astype(F32)
        exits += exit_ref[k].astype(F32)
    small = pair(exits[GROUP_ROWS:, 0:128] + exits[GROUP_ROWS:, 128:256])
    for z in range(DEPTH):
        rows = slice(z * PADDED, (z + 1) * PADDED)
        out_ref[z] = jnp.concatenate([lined(exits[rows]), lined(heads[rows]), small], axis=0)


def finish_kernel(in_ref, exit_ref, head_ref, tiles_ref):
    total = sum(in_ref[z].astype(F32) for z in range(DEPTH))
    exit_ref[...] = total[0:PADDED]
    head_ref[...] = total[SMALL : SMALL + PADDED]
    small = total[2 * SMALL :, 0:128] + total[2 * SMALL :, 128:256]
    for k in range(GROUPS):
        tiles_ref[k] = small


def exact(dims):
    def dot(a, b):
        return lax.dot_general(a, b, (dims, ((), ())), precision=lax.Precision.HIGHEST, preferred_element_type=F32)

    return dot


def last_kernel(
    tiles_ref, embed_ref, gains_ref, pos_ref, wq_ref, wk_ref, wv_ref, exit_ref, head_ref, q_ref, k_ref, v_ref, rest_ref
):
    basis = jnp.concatenate([embed_ref[...].astype(F32), pos_ref[...]], axis=0)
    scaled = basis * gains_ref[0:1, :].astype(F32)
    total = from_tiles(tiles_ref)
    scaled_grad = exact(((0,), (0,)))(scaled, total)
    plain_grad = exact(((0,), (0,)))(basis, total)
    embed = jnp.zeros((OWN, PATCH), F32)
    gain_zero = jnp.zeros((OWN, 1), F32)
    for w, (weight_ref, out_ref) in enumerate(((wq_ref, q_ref), (wk_ref, k_ref), (wv_ref, v_ref))):
        weight = weight_ref[...].astype(F32)
        out_ref[...] = scaled_grad[:, w * WIDE : w * WIDE + COLS]
        gain_zero += jnp.sum(weight * plain_grad[:, w * WIDE : w * WIDE + COLS], axis=1, keepdims=True)
        embed += exact(((1,), (1,)))(weight, total[0:PATCH, w * WIDE : w * WIDE + COLS])
    pick = (lax.broadcasted_iota(jnp.int32, (2, PATCH), 0) == 0).astype(F32)
    embed = embed * exact(((0,), (0,)))(gains_ref[...].astype(F32), pick)
    mixed = jnp.concatenate([tiles_ref[TILES + i] for i in range(BASIS // 8)], axis=0)[:, 0:PATCH]
    embed = embed - exact(((0,), (0,)))(basis, mixed)
    ends = exit_ref[0:OWN, COLS : COLS + PATCH] + exit_ref[0:OWN, COLS + PATCH : WIDE]
    gain_one = head_ref[0:OWN, COLS : COLS + 1] + head_ref[0:OWN, COLS + 1 : COLS + 2]
    loss = jnp.sum(tiles_ref[TILES + BASIS // 8][0:1, :], axis=1, keepdims=True)
    rest_ref[...] = jnp.zeros_like(rest_ref)
    rest_ref[0:OWN, 0:PATCH] = embed + 0.25 * ends
    rest_ref[0:OWN, PATCH : PATCH + 1] = gain_zero
    rest_ref[0:OWN, PATCH + 1 : PATCH + 2] = gain_one
    rest_ref[0:1, PATCH + 2 : PATCH + 3] = loss


def swapped(x, axis):
    return lax.ppermute(x, axis, [(0, 1), (1, 0)])


def mp_sum(mine, other):
    half = (mine.astype(F32) + swapped(other, "mp_1").astype(F32)).astype(BF)
    half = (half.astype(F32) + swapped(half, "mp_0").astype(F32)).astype(BF)
    return half, swapped(half, "mp_1")


def over(x, axis):
    return lax.all_to_all(x, axis, 0, 0, tiled=True)


def padded_rows(x):
    return jnp.pad(x, ((0, PADDED - OWN), (0, WIDE - x.shape[1])))


def prepare(history, later):
    number = history.shape[0]
    centre = jnp.mean(history, axis=1, keepdims=True)
    spread = jnp.sqrt(jnp.mean((history - centre) * (history - centre), axis=1, keepdims=True) + STAT_EPS)
    normed = (history - centre) / spread
    ahead = (later - centre) / spread
    joined = jnp.concatenate([normed, ahead], axis=1).reshape(number, -1, PATCH)
    member = lax.axis_index(MP)
    target = lax.dynamic_slice_in_dim(joined, member + 1, PATCHES, 1).reshape(number * PATCHES, PATCH)
    patches = joined[:, :PATCHES].reshape(number * PATCHES, PATCH).astype(BF)
    return patches.T, target.T


def per_device(history, later, embed, gains, asking, lookup, content, attend_exit, outlook):
    place = lax.axis_index(DP)
    pos = lax.dynamic_index_in_dim(jnp.asarray(position_table()), place, 0, keepdims=False)
    pos_high, pos_low = two(pos)
    exit_block = padded_rows(jnp.concatenate([attend_exit.T, embed.T, pos_high.T, pos_low.T], axis=1))
    head_block = padded_rows(jnp.concatenate([outlook, gains.T], axis=1))

    tiles = call(basis_kernel, [((BLOCKS, 8, 128), F32)], embed, gains, pos, asking, lookup, content)[0]
    tiles = over(tiles.reshape(GROUPS, SMALL, 128), XY)
    packed = ((DEPTH, 3 * SMALL, WIDE), BF)
    with_small = ((GROUPS, GROUP_ROWS + SMALL, WIDE), BF)
    without = ((GROUPS, GROUP_ROWS, WIDE), BF)
    stacked = over(call(blocks_out_kernel, [packed], tiles, exit_block, head_block)[0], Z)
    exit_all, head_all = call(column_kernel, [with_small, without], stacked)
    exit_all = over(exit_all, XY)
    head_all = over(head_all, XY)

    patches, target = prepare(history, later)
    number = np.arange(TOKENS) % PATCHES
    place_hot = jnp.asarray((np.arange(PATCHES)[:, None] == number[None, :]), dtype=BF)
    basis = jnp.concatenate([patches, place_hot, place_hot], axis=0)

    turned = (COLS, TOKENS)
    half = ((HALF, TOKENS), BF)
    mine, other, context, queries, keys, values, probs, factor_zero = call(
        attention_kernel,
        [
            half,
            half,
            (turned, BF),
            (turned, BF),
            (turned, BF),
            (turned, BF),
            ((COLS // HEAD_DIM, TOKENS, TOKENS), F32),
            ((8, TOKENS), F32),
        ],
        exit_all,
        basis,
    )
    mine, other = mp_sum(mine, other)
    mine, other, head_grad, residual, factor_one, loss = call(
        head_kernel,
        [half, half, without, ((ROWS, TOKENS), F32), ((8, TOKENS), F32), ((8, TOKENS), F32)],
        exit_all,
        head_all,
        basis,
        mine,
        other,
        target,
    )
    head_grad = over(head_grad, XY)
    mine, other = mp_sum(mine, other)
    exit_grad = call(
        backward_kernel,
        [with_small],
        exit_all,
        head_all,
        basis,
        mine,
        other,
        residual,
        factor_one,
        factor_zero,
        context,
        queries,
        keys,
        values,
        probs,
        loss,
    )[0]
    exit_grad = over(exit_grad, XY)
    stacked = over(call(scatter_kernel, [packed], head_grad, exit_grad)[0], Z)
    block = ((PADDED, WIDE), F32)
    exit_sum, head_sum, totals = call(finish_kernel, [block, block, ((GROUPS, SMALL, 128), F32)], stacked)
    totals = over(totals, XY).reshape(BLOCKS, 8, 128)
    own = (OWN, COLS)
    query_grad, key_grad, value_grad, rest = call(
        last_kernel,
        [(own, F32), (own, F32), (own, F32), ((PADDED, 128), F32)],
        totals,
        embed,
        gains,
        pos,
        asking,
        lookup,
        content,
        exit_sum,
        head_sum,
    )
    rest = rest + swapped(rest, "mp_1")
    rest = rest + swapped(rest, "mp_0")
    loss_mean = rest[0, PATCH + 2] / 1048576.0
    return (
        loss_mean,
        rest[:OWN, :PATCH].T,
        rest[:OWN, PATCH : PATCH + 2].T,
        query_grad,
        key_grad,
        value_grad,
        exit_sum[:OWN, :COLS].T,
        head_sum[:OWN, :COLS],
    )


def solution(mesh):
    split = Mesh(mesh.devices.reshape(4, 4, 4, 2, 2), ("dp_0", "dp_1", "dp_2", "mp_0", "mp_1"))
    placed = (
        P(DP, None),
        P(DP, None),
        P(None, DP),
        P(None, DP),
        P(DP, MP),
        P(DP, MP),
        P(DP, MP),
        P(MP, DP),
        P(DP, MP),
    )
    return jax.shard_map(
        per_device,
        mesh=split,
        in_specs=placed,
        out_specs=(
            P(),
            P(None, DP),
            P(None, DP),
            P(DP, MP),
            P(DP, MP),
            P(DP, MP),
            P(MP, DP),
            P(DP, MP),
        ),
        check_vma=False,
    )
```

```python
import math

import jax
import jax.numpy as jnp
import numpy as np
from jax import lax
from jax.experimental import pallas as pl
from jax.experimental.pallas import tpu as pltpu
from jax.sharding import Mesh
from jax.sharding import PartitionSpec as P

WIDTH = 1280
PATCH = 32
PATCHES = 16
HEAD_DIM = 80
CHANNELS = 10
BLOCKS = 64
OWN = WIDTH // BLOCKS
TOKENS = 128
COLS = 320
WIDE = 384
BASIS = PATCH + PATCHES
TILES = (BASIS // 8) * (3 * WIDE // 128)
DP = ("dp_0", "dp_1", "dp_2")
XY = ("dp_0", "dp_2")
Z = "dp_1"
GROUPS = 16
DEPTH = 4
GROUP_ROWS = DEPTH * OWN
SMALL = 8 * BLOCKS // GROUPS
LINED = 32
FIRST = [(0, 1), (1, 0), (2, 3), (3, 2)]
SECOND = [(0, 3), (3, 0), (1, 2), (2, 1)]
HALF = WIDTH // 2
MP = ("mp_0", "mp_1")
EPS = 1e-06
STAT_EPS = 1e-05
RADIUS = 0.05
SCALE = 1.0 / math.sqrt(HEAD_DIM)
GRANT = 24 * 1024 * 1024
BF = jnp.bfloat16
F32 = jnp.float32


def nn(a, b):
    return lax.dot_general(a, b, (((1,), (0,)), ((), ())), preferred_element_type=F32)


def nt(a, b):
    return lax.dot_general(a, b, (((1,), (1,)), ((), ())), preferred_element_type=F32)


def tn(a, b):
    return lax.dot_general(a, b, (((0,), (0,)), ((), ())), preferred_element_type=F32)


def two(x):
    high = x.astype(BF)
    return high, (x - high.astype(F32)).astype(BF)


def position_table():
    half = WIDTH // 2
    freqs = np.exp(np.float32(-math.log(10000.0)) * np.arange(half, dtype=np.float32) / np.float32(half))
    angles = np.arange(PATCHES, dtype=np.float32)[:, None] * freqs[None, :]
    table = np.concatenate([np.sin(angles), np.cos(angles)], axis=1).astype(np.float32)
    return np.ascontiguousarray(table.reshape(PATCHES, BLOCKS, OWN).transpose(1, 0, 2))


def turned_table():
    table = position_table().transpose(0, 2, 1)
    high = table.astype(jnp.bfloat16)
    low = (table - high.astype(np.float32)).astype(jnp.bfloat16)
    return np.concatenate([high, low], axis=2)


def call(body, outs, *args, grant=GRANT):
    return pl.pallas_call(
        body,
        out_shape=[jax.ShapeDtypeStruct(s, d) for s, d in outs],
        name=body.__name__,
        compiler_params=pltpu.CompilerParams(vmem_limit_bytes=grant),
    )(*args)


def own_basis(embed_ref, table_ref):
    eye = lax.broadcasted_iota(jnp.int32, (PATCH, PATCH), 0) == lax.broadcasted_iota(jnp.int32, (PATCH, PATCH), 1)
    embed = nt(eye.astype(F32).astype(BF), embed_ref[...])
    return jnp.concatenate([embed, table_ref[lax.axis_index(DP)]], axis=0)


def basis_kernel(
    embed_ref, gains_ref, table_ref, turned_ref, wq_ref, wk_ref, wv_ref, exit_ref, head_ref, out_ref, block_ref
):
    high, low = two(own_basis(embed_ref, table_ref) * gains_ref[0:1, :].astype(F32))
    out_ref[...] = jnp.zeros_like(out_ref)
    for w, ref in enumerate((wq_ref, wk_ref, wv_ref)):
        weight = ref[...]
        part = nn(high, weight) + nn(low, weight)
        for i in range(BASIS // 8):
            rows = part[8 * i : 8 * i + 8]
            for j in range(3):
                at = 9 * i + 3 * w + j
                lanes = rows[:, 128 * j : min(128 * j + 128, COLS)]
                k, t = at // DEPTH, 8 * (at % DEPTH)
                out_ref[k, t : t + 8, 0 : lanes.shape[1]] = lanes
    pair_eye = lax.broadcasted_iota(jnp.int32, (2, 2), 0) == lax.broadcasted_iota(jnp.int32, (2, 2), 1)
    block_ref[...] = jnp.zeros_like(block_ref)
    block_ref[0:OWN, 0:COLS] = exit_ref[...]
    block_ref[0:OWN, COLS : COLS + PATCH] = embed_ref[...]
    block_ref[0:OWN, COLS + PATCH : WIDE] = turned_ref[lax.axis_index(DP)]
    block_ref[LINED : LINED + OWN, 0:COLS] = head_ref[...]
    block_ref[LINED : LINED + OWN, COLS : COLS + 2] = tn(gains_ref[...], pair_eye.astype(F32).astype(BF)).astype(BF)


def from_tiles(ref):
    def tile(at):
        return ref[at // DEPTH, 8 * (at % DEPTH) : 8 * (at % DEPTH) + 8, :]

    return jnp.concatenate(
        [jnp.concatenate([tile(9 * i + j) for j in range(9)], axis=1) for i in range(BASIS // 8)], axis=0
    )


def blocks(ref, lanes=slice(0, WIDE)):
    rows = ref[:, :, lanes]
    return rows.reshape(WIDTH, rows.shape[2])


def spread_halves(value, mine_ref, other_ref):
    north = lax.axis_index("mp_1") == 1
    mine_ref[...] = jnp.where(north, value[HALF:], value[:HALF]).astype(BF)
    other_ref[...] = jnp.where(north, value[:HALF], value[HALF:]).astype(BF)


def joined_halves(mine_ref, other_ref):
    north = lax.axis_index("mp_1") == 1
    mine, other = mine_ref[...].astype(F32), other_ref[...].astype(F32)
    return jnp.concatenate([jnp.where(north, other, mine), jnp.where(north, mine, other)], axis=0)


def raw_projections(tiles_ref, basis):
    high, low = two(from_tiles(tiles_ref))
    return tn(jnp.concatenate([high, low], axis=0), jnp.concatenate([basis, basis], axis=0))


def first_residual(exit_ref, basis_ref):
    lanes = blocks(exit_ref, slice(256, 384))
    entries = basis_ref[...]
    return nn(lanes, jnp.concatenate([jnp.zeros_like(entries), entries], axis=0))


def causal_mask():
    j = lax.broadcasted_iota(jnp.int32, (TOKENS, TOKENS), 0)
    i = lax.broadcasted_iota(jnp.int32, (TOKENS, TOKENS), 1)
    same = lax.shift_right_logical(j, 4) == lax.shift_right_logical(i, 4)
    return same & (j <= i)


def attention_kernel(
    exit_ref, tiles_ref, basis_ref, mine_ref, other_ref, context_ref, queries_ref, keys_ref, values_ref, probs_ref, factor_ref
):
    residual = first_residual(exit_ref, basis_ref)
    factor = lax.rsqrt(jnp.sum(residual * residual, axis=0, keepdims=True) / WIDTH + EPS)
    factor_ref[...] = jnp.broadcast_to(factor, factor_ref.shape)
    raw = raw_projections(tiles_ref, basis_ref[0:BASIS, :]) * factor
    queries_ref[...] = raw[0:COLS].astype(BF)
    keys_ref[...] = raw[WIDE : WIDE + COLS].astype(BF)
    values_ref[...] = raw[2 * WIDE : 2 * WIDE + COLS].astype(BF)
    mask = causal_mask()
    for h in range(COLS // HEAD_DIM):
        at = slice(h * HEAD_DIM, (h + 1) * HEAD_DIM)
        scores = tn(keys_ref[at, :], queries_ref[at, :]) * SCALE
        raised = jnp.where(mask, jnp.exp(scores), 0.0)
        probs = raised / jnp.sum(raised, axis=0, keepdims=True)
        probs_ref[h] = probs
        context_ref[at, :] = nn(values_ref[at, :], probs.astype(BF)).astype(BF)
    context = jnp.concatenate([context_ref[...], jnp.zeros((WIDE - COLS, TOKENS), BF)], axis=0)
    spread_halves(nn(blocks(exit_ref), context), mine_ref, other_ref)


def head_kernel(
    exit_ref,
    head_ref,
    basis_ref,
    half_ref,
    rest_ref,
    target_ref,
    mine_ref,
    other_ref,
    grad_ref,
    residual_ref,
    factor_ref,
    loss_ref,
):
    head = blocks(head_ref)
    residual = first_residual(exit_ref, basis_ref) + joined_halves(half_ref, rest_ref)
    residual_ref[...] = residual
    factor = lax.rsqrt(jnp.sum(residual * residual, axis=0, keepdims=True) / WIDTH + EPS)
    factor_ref[...] = jnp.broadcast_to(factor, factor_ref.shape)
    scaled = residual * factor
    normed = (scaled * head[:, COLS + 1 : COLS + 2].astype(F32)).astype(BF)
    forecast = tn(head, normed)[0:COLS]
    column = lax.broadcasted_iota(jnp.int32, (COLS, 1), 0).astype(F32)
    step = jnp.floor((column + 0.5) * 0.1)
    channel = column - CHANNELS * step
    spread = (step == lax.broadcasted_iota(jnp.int32, (COLS, PATCH), 1).astype(F32)).astype(F32).astype(BF)
    target = target_ref[...]
    first, rest = target.astype(BF), target
    rest = rest - first.astype(F32)
    second, third = two(rest)
    expanded = nn(spread, first) + (nn(spread, second) + nn(spread, third))
    error = expanded - forecast
    share = channel / CHANNELS
    mean_channel = channel == 0.0
    inside = error / -RADIUS
    tail = jnp.exp(-jnp.abs(inside))
    softplus = jnp.maximum(inside, 0.0) + jnp.log1p(tail)
    sigmoid = jnp.where(inside >= 0.0, 1.0, tail) / (1.0 + tail)
    terms = jnp.where(mean_channel, error * error, share * error + RADIUS * softplus)
    loss_ref[...] = jnp.broadcast_to(jnp.sum(terms, axis=0, keepdims=True), loss_ref.shape)
    slope = (jnp.where(mean_channel, -2.0 * error, sigmoid - share) * (1.0 / 128.0)).astype(BF)
    slope = jnp.concatenate([slope, jnp.zeros((WIDE - COLS, TOKENS), BF)], axis=0)
    back = nn(head, slope)
    spread_halves(back, mine_ref, other_ref)
    high, low = two(jnp.sum(back * scaled, axis=1, keepdims=True))
    lane = lax.broadcasted_iota(jnp.int32, (1, WIDE), 1)
    grad = nt(normed, slope)
    grad = jnp.where(lane == COLS, high.astype(F32), jnp.where(lane == COLS + 1, low.astype(F32), grad))
    grad_ref[...] = grad.astype(BF).reshape(GROUPS, GROUP_ROWS, WIDE)


def backward_kernel(
    exit_ref,
    head_ref,
    tiles_ref,
    basis_ref,
    half_ref,
    rest_ref,
    residual_ref,
    factor_one_ref,
    factor_zero_ref,
    context_ref,
    queries_ref,
    keys_ref,
    values_ref,
    probs_ref,
    loss_ref,
    grad_ref,
    out_ref,
):
    basis = basis_ref[0:BASIS, :]
    patches = basis_ref[0:PATCH, :]
    upstream = joined_halves(half_ref, rest_ref)
    residual = residual_ref[...]
    factor = factor_one_ref[0:1, :]
    weighted = blocks(head_ref, slice(256, 384))[:, COLS - 255 : COLS - 254].astype(F32) * upstream
    inner = jnp.sum(weighted * residual, axis=0, keepdims=True) / WIDTH
    low = (factor * weighted - residual * (factor * factor * factor * inner)).astype(BF)
    grad = nt(low, jnp.concatenate([context_ref[...], patches, patches], axis=0))
    lane = lax.broadcasted_iota(jnp.int32, (1, WIDE), 1)
    grad = jnp.where(lane >= COLS + PATCH, grad - grad.astype(BF).astype(F32), grad)
    grad_ref[...] = grad.astype(BF).reshape(GROUPS, GROUP_ROWS, WIDE)
    context_grad = tn(blocks(exit_ref), low)[0:COLS].astype(BF)
    backs = ([], [], [])
    for h in range(COLS // HEAD_DIM):
        at = slice(h * HEAD_DIM, (h + 1) * HEAD_DIM)
        slope = context_grad[at]
        probs = probs_ref[h]
        prob_grad = tn(values_ref[at, :], slope)
        value_back = nt(slope, probs.astype(BF))
        centred = prob_grad - jnp.sum(probs * prob_grad, axis=0, keepdims=True)
        score_grad = (probs * centred * SCALE).astype(BF)
        backs[0].append(nn(keys_ref[at, :], score_grad).astype(BF))
        backs[1].append(nt(queries_ref[at, :], score_grad).astype(BF))
        backs[2].append(value_back.astype(BF))
    gap = jnp.zeros((WIDE - COLS, TOKENS), BF)
    back = jnp.concatenate([*backs[0], gap, *backs[1], gap, *backs[2], gap], axis=0)
    factor = factor_zero_ref[0:1, :]
    entries = basis.astype(F32)
    high, low = two(entries * factor)
    total = nt(high, back) + nt(low, back)
    raw = raw_projections(tiles_ref, basis)
    inner = jnp.sum(back.astype(F32) * raw, axis=0, keepdims=True) / WIDTH
    high, low = two(entries * (factor * factor * factor * inner))
    mixed = nt(high, patches) + nt(low, patches)
    blank = jnp.zeros((8, 128 - PATCH), F32)
    tiles = [total[8 * i : 8 * i + 8, 128 * j : 128 * j + 128] for i in range(BASIS // 8) for j in range(9)]
    tiles += [jnp.concatenate([mixed[8 * i : 8 * i + 8], blank], axis=1) for i in range(BASIS // 8)]
    tiles += [loss_ref[...]]
    tiles += [jnp.zeros((8, 128), F32)] * (BLOCKS - len(tiles))
    for k in range(GROUPS):
        out_ref[k] = jnp.concatenate(tiles[DEPTH * k : DEPTH * k + DEPTH], axis=0)


def group_sum(ref):
    total = ref[0].astype(F32)
    for k in range(1, GROUPS):
        total += ref[k].astype(F32)
    return total


def gather_kernel(tiles_ref, own_ref, next_ref, far_ref, total_ref, exit_ref, head_ref):
    total_ref[...] = group_sum(tiles_ref)
    own, near, far = (ref[...].astype(F32) for ref in (own_ref, next_ref, far_ref))
    parts = [own, near, far[: 2 * LINED], far[2 * LINED :]]
    exits = jnp.concatenate([p[0:OWN] for p in parts], axis=0).astype(BF)
    heads = jnp.concatenate([p[LINED : LINED + OWN] for p in parts], axis=0).astype(BF)
    for k in range(GROUPS):
        exit_ref[k] = exits
        head_ref[k] = heads


def total_kernel(one_ref, other_ref, out_ref):
    total = one_ref[...] + other_ref[...]
    for k in range(GROUPS):
        out_ref[k] = total


def exact(dims):
    def dot(a, b):
        return lax.dot_general(a, b, (dims, ((), ())), precision=lax.Precision.HIGHEST, preferred_element_type=F32)

    return dot


def last_kernel(
    tiles_ref,
    embed_ref,
    gains_ref,
    table_ref,
    wq_ref,
    wk_ref,
    wv_ref,
    exit_ref,
    head_ref,
    q_ref,
    k_ref,
    v_ref,
    exit_grad_ref,
    head_grad_ref,
    rest_ref,
):
    basis = own_basis(embed_ref, table_ref)
    total = from_tiles(tiles_ref)
    scaled_grad = exact(((0,), (0,)))(basis * gains_ref[0:1, :].astype(F32), total)
    plain_grad = exact(((0,), (0,)))(basis, total)
    embed = jnp.zeros((OWN, PATCH), F32)
    gain_zero = jnp.zeros((OWN, 1), F32)
    for w, (weight_ref, grad_ref) in enumerate(((wq_ref, q_ref), (wk_ref, k_ref), (wv_ref, v_ref))):
        weight = weight_ref[...].astype(F32)
        grad_ref[...] = scaled_grad[:, w * WIDE : w * WIDE + COLS]
        gain_zero += jnp.sum(weight * plain_grad[:, w * WIDE : w * WIDE + COLS], axis=1, keepdims=True)
        embed += exact(((1,), (1,)))(weight, total[0:PATCH, w * WIDE : w * WIDE + COLS])
    pick = (lax.broadcasted_iota(jnp.int32, (2, PATCH), 0) == 0).astype(F32)
    embed = embed * exact(((0,), (0,)))(gains_ref[...].astype(F32), pick)

    def small(at):
        return tiles_ref[at // DEPTH, 8 * (at % DEPTH) : 8 * (at % DEPTH) + 8, :]

    mixed = jnp.concatenate([small(TILES + i) for i in range(BASIS // 8)], axis=0)[:, 0:PATCH]
    embed = embed - exact(((0,), (0,)))(basis, mixed)
    ends = exit_ref[:, COLS : COLS + PATCH] + exit_ref[:, COLS + PATCH : WIDE]
    gain_one = head_ref[:, COLS : COLS + 1] + head_ref[:, COLS + 1 : COLS + 2]
    exit_grad_ref[...] = exit_ref[:, 0:COLS]
    head_grad_ref[...] = head_ref[:, 0:COLS]
    rest_ref[...] = jnp.zeros_like(rest_ref)
    rest_ref[0:OWN, 0:PATCH] = embed + 0.25 * ends
    rest_ref[0:OWN, PATCH : PATCH + 1] = gain_zero
    rest_ref[0:OWN, PATCH + 1 : PATCH + 2] = gain_one
    rest_ref[0:1, PATCH + 2 : PATCH + 3] = jnp.sum(small(TILES + BASIS // 8)[0:1, :], axis=1, keepdims=True)


def end_kernel(one_ref, other_ref, embed_ref, gains_ref, loss_ref):
    rest = one_ref[...] + other_ref[...]
    embed_ref[...] = rest[0:OWN, 0:PATCH]
    gains_ref[...] = rest.T[PATCH : PATCH + 2, 0:OWN]
    loss_ref[...] = rest[0:1, PATCH + 2 : PATCH + 3] / 1048576.0


def swapped(x, axis):
    return lax.ppermute(x, axis, [(0, 1), (1, 0)])


def mp_sum(mine, other):
    half = (mine.astype(F32) + swapped(other, "mp_1").astype(F32)).astype(BF)
    half = (half.astype(F32) + swapped(half, "mp_0").astype(F32)).astype(BF)
    return half, swapped(half, "mp_1")


def over(x, axis):
    return lax.all_to_all(x, axis, 0, 0, tiled=True)


def along_z(x, pairs):
    return lax.ppermute(x, Z, pairs)


def to_owner(x):
    kept = x[: 2 * OWN] + along_z(x[2 * OWN :].astype(BF), SECOND).astype(F32)
    return kept[:OWN] + along_z(kept[OWN:].astype(BF), FIRST).astype(F32)


def after(x, *others):
    return lax.optimization_barrier((x, *others))[0]


def prepare(history, later):
    number = history.shape[0]
    centre = jnp.mean(history, axis=1, keepdims=True)
    spread = jnp.sqrt(jnp.mean((history - centre) * (history - centre), axis=1, keepdims=True) + STAT_EPS)
    normed = (history - centre) / spread
    ahead = (later - centre) / spread
    joined = jnp.concatenate([normed, ahead], axis=1).reshape(number, -1, PATCH)
    member = lax.axis_index(MP)
    target = lax.dynamic_slice_in_dim(joined, member + 1, PATCHES, 1).reshape(number * PATCHES, PATCH)
    patches = joined[:, :PATCHES].reshape(number * PATCHES, PATCH).astype(BF)
    return patches.T, target.T


def per_device(history, later, embed, gains, asking, lookup, content, attend_exit, outlook):
    table = jnp.asarray(position_table())
    embed_turned = embed.T
    tiles_like = ((GROUPS, SMALL, 128), F32)
    groups = ((GROUPS, GROUP_ROWS, WIDE), BF)
    tiles, block = call(
        basis_kernel,
        [tiles_like, ((2 * LINED, WIDE), BF)],
        embed_turned,
        gains,
        table,
        jnp.asarray(turned_table()),
        asking,
        lookup,
        content,
        attend_exit.T,
        outlook,
        grant=None,
    )
    tiles = over(tiles, XY)
    near = along_z(block, FIRST)
    far = along_z(jnp.concatenate([block, near], axis=0), SECOND)
    total, exit_all, head_all = call(
        gather_kernel, [((SMALL, 128), F32), groups, groups], tiles, block, near, far
    )
    exit_all = over(exit_all, XY)
    total = total + along_z(total, FIRST)
    tiles = call(total_kernel, [tiles_like], total, along_z(total, SECOND))[0]

    patches, target = prepare(history, later)
    number = np.arange(TOKENS) % PATCHES
    place_hot = jnp.asarray((np.arange(PATCHES)[:, None] == number[None, :]), dtype=BF)
    basis = jnp.concatenate([patches, place_hot, place_hot], axis=0)
    tiles, exit_all, basis, target = lax.optimization_barrier((tiles, exit_all, basis, target))
    tiles = over(tiles, XY)
    head_all = over(after(head_all, tiles), XY)

    turned = (COLS, TOKENS)
    half = ((HALF, TOKENS), BF)
    mine, other, context, queries, keys, values, probs, factor_zero = call(
        attention_kernel,
        [
            half,
            half,
            (turned, BF),
            (turned, BF),
            (turned, BF),
            (turned, BF),
            ((COLS // HEAD_DIM, TOKENS, TOKENS), F32),
            ((8, TOKENS), F32),
        ],
        exit_all,
        tiles,
        basis,
    )
    mine, other = mp_sum(mine, other)
    mine, other, head_grad, residual, factor_one, loss = call(
        head_kernel,
        [half, half, groups, ((WIDTH, TOKENS), F32), ((8, TOKENS), F32), ((8, TOKENS), F32)],
        exit_all,
        head_all,
        basis,
        mine,
        other,
        target,
    )
    head_grad = over(head_grad, XY)
    mine, other = mp_sum(mine, other)
    exit_grad, totals = call(
        backward_kernel,
        [groups, tiles_like],
        exit_all,
        head_all,
        tiles,
        basis,
        mine,
        other,
        residual,
        factor_one,
        factor_zero,
        context,
        queries,
        keys,
        values,
        probs,
        loss,
    )
    totals = over(after(totals, head_grad), XY)
    head_sum = to_owner(jnp.sum(head_grad.astype(F32), axis=0))
    exit_grad = over(after(exit_grad, totals), XY)
    total = jnp.sum(totals, axis=0)
    total = total + along_z(total, FIRST)
    totals = call(total_kernel, [tiles_like], total, along_z(total, SECOND))[0]
    totals = over(after(totals, exit_grad), XY)
    exit_sum = to_owner(jnp.sum(exit_grad.astype(F32), axis=0))
    own = ((OWN, COLS), F32)
    query_grad, key_grad, value_grad, output_grad, head_weight_grad, rest = call(
        last_kernel,
        [own, own, own, own, own, ((24, 128), F32)],
        totals,
        embed_turned,
        gains,
        table,
        asking,
        lookup,
        content,
        exit_sum,
        head_sum,
    )
    rest = rest + swapped(rest, "mp_1")
    embed_grad, gains_grad, loss_mean = call(
        end_kernel,
        [((OWN, PATCH), F32), ((2, OWN), F32), ((1, 1), F32)],
        rest,
        swapped(rest, "mp_0"),
    )
    return (
        loss_mean[0, 0],
        embed_grad.T,
        gains_grad,
        query_grad,
        key_grad,
        value_grad,
        output_grad.T,
        head_weight_grad,
    )


def solution(mesh):
    split = Mesh(mesh.devices.reshape(4, 4, 4, 2, 2), ("dp_0", "dp_1", "dp_2", "mp_0", "mp_1"))
    placed = (
        P(DP, None),
        P(DP, None),
        P(None, DP),
        P(None, DP),
        P(DP, MP),
        P(DP, MP),
        P(DP, MP),
        P(MP, DP),
        P(DP, MP),
    )
    return jax.shard_map(
        per_device,
        mesh=split,
        in_specs=placed,
        out_specs=(
            P(),
            P(None, DP),
            P(None, DP),
            P(DP, MP),
            P(DP, MP),
            P(DP, MP),
            P(MP, DP),
            P(DP, MP),
        ),
        check_vma=False,
    )
```

```python
import math

import jax
import jax.numpy as jnp
import numpy as np
from jax import lax
from jax.experimental import pallas as pl
from jax.experimental.pallas import tpu as pltpu
from jax.sharding import Mesh
from jax.sharding import PartitionSpec as P


WIDTH = 1280
PATCH = 32
PATCHES = 16
HEAD_DIM = 80
CHANNELS = 10
BLOCKS = 64
OWN = WIDTH // BLOCKS
TOKENS = 128
COLS = 320
WIDE = 384
BASIS = PATCH + PATCHES
TILES = (BASIS // 8) * (3 * WIDE // 128)
DP = ("dp_0", "dp_1", "dp_2")
XY = ("dp_0", "dp_2")
Z = "dp_1"
GROUPS = 16
DEPTH = 4
GROUP_ROWS = DEPTH * OWN
SMALL = 8 * BLOCKS // GROUPS
LINED = 32
FIRST = [(0, 1), (1, 0), (2, 3), (3, 2)]
SECOND = [(0, 3), (3, 0), (1, 2), (2, 1)]
FOURTH = [(0, 2), (2, 0), (1, 3), (3, 1)]
HALF = WIDTH // 2
MP = ("mp_0", "mp_1")
HEADS = [slice(at, at + HEAD_DIM) for at in range(0, COLS, HEAD_DIM)]
EPS = 1e-06
STAT_EPS = 1e-05
RADIUS = 0.05
SCALE = 1.0 / math.sqrt(HEAD_DIM)
GRANT = 16 * 1024 * 1024
BF = jnp.bfloat16
F32 = jnp.float32


def nn(a, b):
    return lax.dot_general(a, b, (((1,), (0,)), ((), ())), preferred_element_type=F32)


def nt(a, b):
    return lax.dot_general(a, b, (((1,), (1,)), ((), ())), preferred_element_type=F32)


def tn(a, b):
    return lax.dot_general(a, b, (((0,), (0,)), ((), ())), preferred_element_type=F32)


def two(x):
    high = x.astype(BF)
    return high, (x - high.astype(F32)).astype(BF)


def position_table():
    half = WIDTH // 2
    freqs = np.exp(np.float32(-math.log(10000.0)) * np.arange(half, dtype=np.float32) / np.float32(half))
    angles = np.arange(PATCHES, dtype=np.float32)[:, None] * freqs[None, :]
    table = np.concatenate([np.sin(angles), np.cos(angles)], axis=1).astype(np.float32)
    return np.ascontiguousarray(table.reshape(PATCHES, BLOCKS, OWN).transpose(1, 0, 2))


def turned_table():
    table = position_table().transpose(0, 2, 1)
    high = table.astype(jnp.bfloat16)
    low = (table - high.astype(np.float32)).astype(jnp.bfloat16)
    return np.concatenate([high, low], axis=2)


def call(body, outs, *args, grant=GRANT):
    return pl.pallas_call(
        body,
        out_shape=[jax.ShapeDtypeStruct(s, d) for s, d in outs],
        compiler_params=pltpu.CompilerParams(vmem_limit_bytes=grant),
    )(*args)


def own_basis(embed_ref, table_ref):
    eye = lax.broadcasted_iota(jnp.int32, (PATCH, PATCH), 0) == lax.broadcasted_iota(jnp.int32, (PATCH, PATCH), 1)
    embed = nt(eye.astype(F32).astype(BF), embed_ref[...])
    return jnp.concatenate([embed, table_ref[lax.axis_index(DP)]], axis=0)


def basis_kernel(
    embed_ref, gains_ref, table_ref, turned_ref, wq_ref, wk_ref, wv_ref, exit_ref, head_ref, out_ref, block_ref
):
    high, low = two(own_basis(embed_ref, table_ref) * gains_ref[0:1, :].astype(F32))
    out_ref[...] = jnp.zeros_like(out_ref)
    for w, ref in enumerate((wq_ref, wk_ref, wv_ref)):
        weight = ref[...]
        part = nn(high, weight) + nn(low, weight)
        for i in range(BASIS // 8):
            rows = part[8 * i : 8 * i + 8]
            for j in range(3):
                at = 9 * i + 3 * w + j
                lanes = rows[:, 128 * j : min(128 * j + 128, COLS)]
                k, t = at // DEPTH, 8 * (at % DEPTH)
                out_ref[k, t : t + 8, 0 : lanes.shape[1]] = lanes
    pair_eye = lax.broadcasted_iota(jnp.int32, (2, 2), 0) == lax.broadcasted_iota(jnp.int32, (2, 2), 1)
    block_ref[...] = jnp.zeros_like(block_ref)
    block_ref[0:OWN, 0:COLS] = exit_ref[...]
    block_ref[0:OWN, COLS : COLS + PATCH] = embed_ref[...]
    block_ref[0:OWN, COLS + PATCH : WIDE] = turned_ref[lax.axis_index(DP)]
    block_ref[LINED : LINED + OWN, 0:COLS] = head_ref[...]
    block_ref[LINED : LINED + OWN, COLS : COLS + 2] = tn(gains_ref[...], pair_eye.astype(F32).astype(BF)).astype(BF)


def from_tiles(ref):
    def tile(at):
        return ref[at // DEPTH, 8 * (at % DEPTH) : 8 * (at % DEPTH) + 8, :]

    return jnp.concatenate(
        [jnp.concatenate([tile(9 * i + j) for j in range(9)], axis=1) for i in range(BASIS // 8)], axis=0
    )


def blocks(ref, lanes=slice(0, WIDE)):
    rows = ref[:, :, lanes]
    return rows.reshape(WIDTH, rows.shape[2])


def spread_halves(value, mine_ref, other_ref):
    north = lax.axis_index("mp_1") == 1
    mine_ref[...] = jnp.where(north, value[HALF:], value[:HALF]).astype(BF)
    other_ref[...] = jnp.where(north, value[:HALF], value[HALF:]).astype(BF)


def joined_halves(mine_ref, other_ref):
    north = lax.axis_index("mp_1") == 1
    mine, other = mine_ref[...].astype(F32), other_ref[...].astype(F32)
    return jnp.concatenate([jnp.where(north, other, mine), jnp.where(north, mine, other)], axis=0)


def raw_projections(tiles_ref, basis):
    high, low = two(from_tiles(tiles_ref))
    return tn(jnp.concatenate([high, low], axis=0), jnp.concatenate([basis, basis], axis=0))


def first_residual(exit_ref, basis_ref):
    lanes = blocks(exit_ref, slice(256, 384))
    entries = basis_ref[...]
    return nn(lanes, jnp.concatenate([jnp.zeros_like(entries), entries], axis=0))


def causal_mask():
    j = lax.broadcasted_iota(jnp.int32, (TOKENS, TOKENS), 0)
    i = lax.broadcasted_iota(jnp.int32, (TOKENS, TOKENS), 1)
    same = lax.shift_right_logical(j, 4) == lax.shift_right_logical(i, 4)
    return same & (j <= i)


def attention(exit_ref, tiles_ref, basis_ref):
    residual = first_residual(exit_ref, basis_ref)
    factor = lax.rsqrt(jnp.sum(residual * residual, axis=0, keepdims=True) / WIDTH + EPS)
    raw = raw_projections(tiles_ref, basis_ref[0:BASIS, :])
    queries, keys, values = ((raw[w * WIDE : w * WIDE + COLS] * factor).astype(BF) for w in range(3))
    mask = causal_mask()
    all_probs, context = [], []
    for at in HEADS:
        scores = tn(keys[at], queries[at]) * SCALE
        raised = jnp.where(mask, jnp.exp(scores), 0.0)
        probs = raised / jnp.sum(raised, axis=0, keepdims=True)
        all_probs.append(probs)
        context.append(nn(values[at], probs.astype(BF)).astype(BF))
    return factor, raw, queries, keys, values, all_probs, context


def attention_kernel(exit_ref, tiles_ref, basis_ref, mine_ref, other_ref):
    context = attention(exit_ref, tiles_ref, basis_ref)[-1]
    context = jnp.concatenate([*context, jnp.zeros((WIDE - COLS, TOKENS), BF)], axis=0)
    spread_halves(nn(blocks(exit_ref), context), mine_ref, other_ref)


def head_kernel(
    exit_ref,
    head_ref,
    basis_ref,
    half_ref,
    rest_ref,
    target_ref,
    mine_ref,
    other_ref,
    grad_ref,
    residual_ref,
):
    head = blocks(head_ref)
    residual = first_residual(exit_ref, basis_ref) + joined_halves(half_ref, rest_ref)
    residual_ref[0:WIDTH, :] = residual
    factor = lax.rsqrt(jnp.sum(residual * residual, axis=0, keepdims=True) / WIDTH + EPS)
    scaled = residual * factor
    normed = (scaled * head[:, COLS + 1 : COLS + 2].astype(F32)).astype(BF)
    forecast = tn(head, normed)[0:COLS]
    column = lax.broadcasted_iota(jnp.int32, (COLS, 1), 0).astype(F32)
    step = jnp.floor((column + 0.5) * 0.1)
    channel = column - CHANNELS * step
    spread = (step == lax.broadcasted_iota(jnp.int32, (COLS, PATCH), 1).astype(F32)).astype(F32).astype(BF)
    target = target_ref[...]
    first, rest = target.astype(BF), target
    rest = rest - first.astype(F32)
    second, third = two(rest)
    expanded = nn(spread, first) + (nn(spread, second) + nn(spread, third))
    error = expanded - forecast
    share = channel / CHANNELS
    mean_channel = channel == 0.0
    inside = error / -RADIUS
    tail = jnp.exp(-jnp.abs(inside))
    softplus = jnp.maximum(inside, 0.0) + jnp.log1p(tail)
    sigmoid = jnp.where(inside >= 0.0, 1.0, tail) / (1.0 + tail)
    terms = jnp.where(mean_channel, error * error, share * error + RADIUS * softplus)
    residual_ref[WIDTH:, :] = jnp.broadcast_to(jnp.sum(terms, axis=0, keepdims=True), (8, TOKENS))
    slope = (jnp.where(mean_channel, -2.0 * error, sigmoid - share) * (1.0 / 128.0)).astype(BF)
    slope = jnp.concatenate([slope, jnp.zeros((WIDE - COLS, TOKENS), BF)], axis=0)
    back = nn(head, slope)
    spread_halves(back, mine_ref, other_ref)
    high, low = two(jnp.sum(back * scaled, axis=1, keepdims=True))
    lane = lax.broadcasted_iota(jnp.int32, (1, WIDE), 1)
    grad = nt(normed, slope)
    grad = jnp.where(lane == COLS, high.astype(F32), jnp.where(lane == COLS + 1, low.astype(F32), grad))
    grad_ref[...] = grad.astype(BF).reshape(GROUPS, GROUP_ROWS, WIDE)


def backward_kernel(
    exit_ref,
    head_ref,
    tiles_ref,
    basis_ref,
    half_ref,
    rest_ref,
    residual_ref,
    grad_ref,
    out_ref,
):
    factor_zero, raw, queries, keys, values, all_probs, context = attention(exit_ref, tiles_ref, basis_ref)
    basis = basis_ref[0:BASIS, :]
    patches = basis_ref[0:PATCH, :]
    upstream = joined_halves(half_ref, rest_ref)
    residual = residual_ref[0:WIDTH, :]
    factor = lax.rsqrt(jnp.sum(residual * residual, axis=0, keepdims=True) / WIDTH + EPS)
    weighted = blocks(head_ref, slice(256, 384))[:, COLS - 255 : COLS - 254].astype(F32) * upstream
    inner = jnp.sum(weighted * residual, axis=0, keepdims=True) / WIDTH
    low = (factor * weighted - residual * (factor * factor * factor * inner)).astype(BF)
    grad = nt(low, jnp.concatenate([*context, patches, patches], axis=0))
    lane = lax.broadcasted_iota(jnp.int32, (1, WIDE), 1)
    grad = jnp.where(lane >= COLS + PATCH, grad - grad.astype(BF).astype(F32), grad)
    grad_ref[...] = grad.astype(BF).reshape(GROUPS, GROUP_ROWS, WIDE)
    context_grad = tn(blocks(exit_ref), low)[0:COLS].astype(BF)
    backs = ([], [], [])
    for at, probs in zip(HEADS, all_probs):
        slope = context_grad[at]
        prob_grad = tn(values[at], slope)
        value_back = nt(slope, probs.astype(BF))
        centred = prob_grad - jnp.sum(probs * prob_grad, axis=0, keepdims=True)
        score_grad = (probs * centred * SCALE).astype(BF)
        backs[0].append(nn(keys[at], score_grad).astype(BF))
        backs[1].append(nt(queries[at], score_grad).astype(BF))
        backs[2].append(value_back.astype(BF))
    gap = jnp.zeros((WIDE - COLS, TOKENS), BF)
    back = jnp.concatenate([*backs[0], gap, *backs[1], gap, *backs[2], gap], axis=0)
    factor = factor_zero
    entries = basis.astype(F32)
    high, low = two(entries * factor)
    total = nt(high, back) + nt(low, back)
    inner = jnp.sum(back.astype(F32) * raw, axis=0, keepdims=True) / WIDTH
    high, low = two(entries * (factor * factor * factor * inner))
    mixed = nt(high, patches) + nt(low, patches)
    blank = jnp.zeros((8, 128 - PATCH), F32)
    tiles = [total[8 * i : 8 * i + 8, 128 * j : 128 * j + 128] for i in range(BASIS // 8) for j in range(9)]
    tiles += [jnp.concatenate([mixed[8 * i : 8 * i + 8], blank], axis=1) for i in range(BASIS // 8)]
    tiles += [residual_ref[WIDTH:, :]]
    tiles += [jnp.zeros((8, 128), F32)] * (BLOCKS - len(tiles))
    for k in range(GROUPS):
        out_ref[k] = jnp.concatenate(tiles[DEPTH * k : DEPTH * k + DEPTH], axis=0)


def group_sum(ref):
    total = ref[0].astype(F32)
    for k in range(1, GROUPS):
        total += ref[k].astype(F32)
    return total


def gather_kernel(tiles_ref, own_ref, first_ref, second_ref, fourth_ref, total_ref, exit_ref, head_ref):
    total_ref[...] = group_sum(tiles_ref)
    parts = [ref[...].astype(F32) for ref in (own_ref, first_ref, second_ref, fourth_ref)]
    exits = jnp.concatenate([p[0:OWN] for p in parts], axis=0).astype(BF)
    heads = jnp.concatenate([p[LINED : LINED + OWN] for p in parts], axis=0).astype(BF)
    for k in range(GROUPS):
        exit_ref[k] = exits
        head_ref[k] = heads


def total_kernel(one_ref, other_ref, out_ref):
    total = one_ref[...] + other_ref[...]
    for k in range(GROUPS):
        out_ref[k] = total


def scatter_kernel(exit_ref, head_ref, keep_ref, send_ref):
    exits, heads = group_sum(exit_ref), group_sum(head_ref)
    rows = [x[OWN * at : OWN * at + OWN] for at in range(DEPTH) for x in (exits, heads)]
    keep_ref[...] = jnp.concatenate(rows[:DEPTH], axis=0)
    send_ref[...] = jnp.concatenate(rows[DEPTH:], axis=0).astype(BF)


def exact(dims):
    def dot(a, b):
        return lax.dot_general(a, b, (dims, ((), ())), precision=lax.Precision.HIGHEST, preferred_element_type=F32)

    return dot


def last_kernel(
    tiles_ref,
    embed_ref,
    gains_ref,
    table_ref,
    wq_ref,
    wk_ref,
    wv_ref,
    sums_ref,
    q_ref,
    k_ref,
    v_ref,
    exit_grad_ref,
    head_grad_ref,
    rest_ref,
):
    basis = own_basis(embed_ref, table_ref)
    total = from_tiles(tiles_ref)
    scaled_grad = exact(((0,), (0,)))(basis * gains_ref[0:1, :].astype(F32), total)
    plain_grad = exact(((0,), (0,)))(basis, total)
    embed = jnp.zeros((OWN, PATCH), F32)
    gain_zero = jnp.zeros((OWN, 1), F32)
    for w, (weight_ref, grad_ref) in enumerate(((wq_ref, q_ref), (wk_ref, k_ref), (wv_ref, v_ref))):
        weight = weight_ref[...].astype(F32)
        grad_ref[...] = scaled_grad[:, w * WIDE : w * WIDE + COLS]
        gain_zero += jnp.sum(weight * plain_grad[:, w * WIDE : w * WIDE + COLS], axis=1, keepdims=True)
        embed += exact(((1,), (1,)))(weight, total[0:PATCH, w * WIDE : w * WIDE + COLS])
    pick = (lax.broadcasted_iota(jnp.int32, (2, PATCH), 0) == 0).astype(F32)
    embed = embed * exact(((0,), (0,)))(gains_ref[...].astype(F32), pick)

    def small(at):
        return tiles_ref[at // DEPTH, 8 * (at % DEPTH) : 8 * (at % DEPTH) + 8, :]

    mixed = jnp.concatenate([small(TILES + i) for i in range(BASIS // 8)], axis=0)[:, 0:PATCH]
    embed = embed - exact(((0,), (0,)))(basis, mixed)
    exit_ref, head_ref = sums_ref[0:OWN, :], sums_ref[OWN : 2 * OWN, :]
    ends = exit_ref[:, COLS : COLS + PATCH] + exit_ref[:, COLS + PATCH : WIDE]
    gain_one = head_ref[:, COLS : COLS + 1] + head_ref[:, COLS + 1 : COLS + 2]
    exit_grad_ref[...] = exit_ref[:, 0:COLS]
    head_grad_ref[...] = head_ref[:, 0:COLS]
    rest_ref[...] = jnp.zeros_like(rest_ref)
    rest_ref[0:OWN, 0:PATCH] = embed + 0.25 * ends
    rest_ref[0:OWN, PATCH : PATCH + 1] = gain_zero
    rest_ref[0:OWN, PATCH + 1 : PATCH + 2] = gain_one
    rest_ref[0:1, PATCH + 2 : PATCH + 3] = jnp.sum(small(TILES + BASIS // 8)[0:1, :], axis=1, keepdims=True)


def end_kernel(one_ref, other_ref, embed_ref, gains_ref, loss_ref):
    rest = one_ref[...] + other_ref[...]
    embed_ref[...] = rest[0:OWN, 0:PATCH]
    gains_ref[...] = rest.T[PATCH : PATCH + 2, 0:OWN]
    loss_ref[...] = rest[0:1, PATCH + 2 : PATCH + 3] / 1048576.0


def swapped(x, axis):
    return lax.ppermute(x, axis, [(0, 1), (1, 0)])


def mp_sum(mine, other):
    half = (mine.astype(F32) + swapped(other, "mp_1").astype(F32)).astype(BF)
    half = (half.astype(F32) + swapped(half, "mp_0").astype(F32)).astype(BF)
    return half, swapped(half, "mp_1")


def over(x, axis):
    return lax.all_to_all(x, axis, 0, 0, tiled=True)


def along_z(x, pairs):
    return lax.ppermute(x, Z, pairs)


def z_total(x):
    x = x + along_z(x, FIRST)
    return call(total_kernel, [((GROUPS, SMALL, 128), F32)], x, along_z(x, SECOND))[0]


def after(x, *others):
    return lax.optimization_barrier((x, *others))[0]


def prepare(history, later):
    number = history.shape[0]
    centre = jnp.mean(history, axis=1, keepdims=True)
    spread = jnp.sqrt(jnp.mean((history - centre) * (history - centre), axis=1, keepdims=True) + STAT_EPS)
    normed = (history - centre) / spread
    ahead = (later - centre) / spread
    joined = jnp.concatenate([normed, ahead], axis=1).reshape(number, -1, PATCH)
    member = lax.axis_index(MP)
    target = lax.dynamic_slice_in_dim(joined, member + 1, PATCHES, 1).reshape(number * PATCHES, PATCH)
    patches = joined[:, :PATCHES].reshape(number * PATCHES, PATCH).astype(BF)
    return patches.T, target.T


def per_device(history, later, embed, gains, asking, lookup, content, attend_exit, outlook):
    table = jnp.asarray(position_table())
    embed_turned = embed.T
    tiles_like = ((GROUPS, SMALL, 128), F32)
    groups = ((GROUPS, GROUP_ROWS, WIDE), BF)
    tiles, block = call(
        basis_kernel,
        [tiles_like, ((2 * LINED, WIDE), BF)],
        embed_turned,
        gains,
        table,
        jnp.asarray(turned_table()),
        asking,
        lookup,
        content,
        attend_exit.T,
        outlook,
        grant=None,
    )
    tiles = over(tiles, XY)
    column = [along_z(block, pairs) for pairs in (FIRST, SECOND, FOURTH)]
    total, exit_all, head_all = call(
        gather_kernel, [((SMALL, 128), F32), groups, groups], tiles, block, *column
    )
    exit_all = over(exit_all, XY)
    tiles = z_total(total)

    patches, target = prepare(history, later)
    number = np.arange(TOKENS) % PATCHES
    place_hot = jnp.asarray((np.arange(PATCHES)[:, None] == number[None, :]), dtype=BF)
    basis = jnp.concatenate([patches, place_hot, place_hot], axis=0)
    tiles, exit_all, basis, target = lax.optimization_barrier((tiles, exit_all, basis, target))
    tiles = over(tiles, XY)
    head_all = over(after(head_all, tiles), XY)

    half = ((HALF, TOKENS), BF)
    mine, other = call(attention_kernel, [half, half], exit_all, tiles, basis)
    mine, other = mp_sum(mine, other)
    mine, other, head_grad, residual = call(
        head_kernel,
        [half, half, groups, ((WIDTH + 8, TOKENS), F32)],
        exit_all,
        head_all,
        basis,
        mine,
        other,
        target,
    )
    head_grad = over(head_grad, XY)
    mine, other = mp_sum(mine, other)
    exit_grad, totals = call(
        backward_kernel,
        [groups, tiles_like],
        exit_all,
        head_all,
        tiles,
        basis,
        mine,
        other,
        residual,
    )
    totals = over(after(totals, head_grad), XY)
    exit_grad = over(after(exit_grad, totals), XY)
    totals = z_total(jnp.sum(totals, axis=0))
    totals = over(after(totals, exit_grad), XY)
    rows = (4 * OWN, WIDE)
    keep, send = call(scatter_kernel, [(rows, F32), (rows, BF)], exit_grad, head_grad)
    keep = keep + along_z(send, SECOND).astype(F32)
    sums = keep[: 2 * OWN] + along_z(keep[2 * OWN :].astype(BF), FIRST).astype(F32)
    own = ((OWN, COLS), F32)
    query_grad, key_grad, value_grad, output_grad, head_weight_grad, rest = call(
        last_kernel,
        [own, own, own, own, own, ((24, 128), F32)],
        totals,
        embed_turned,
        gains,
        table,
        asking,
        lookup,
        content,
        sums,
    )
    rest = rest + swapped(rest, "mp_1")
    embed_grad, gains_grad, loss_mean = call(
        end_kernel,
        [((OWN, PATCH), F32), ((2, OWN), F32), ((1, 1), F32)],
        rest,
        swapped(rest, "mp_0"),
    )
    return (
        loss_mean[0, 0],
        embed_grad.T,
        gains_grad,
        query_grad,
        key_grad,
        value_grad,
        output_grad.T,
        head_weight_grad,
    )


def solution(mesh):
    split = Mesh(mesh.devices.reshape(4, 4, 4, 2, 2), ("dp_0", "dp_1", "dp_2", "mp_0", "mp_1"))
    placed = (
        P(DP, None),
        P(DP, None),
        P(None, DP),
        P(None, DP),
        P(DP, MP),
        P(DP, MP),
        P(DP, MP),
        P(MP, DP),
        P(DP, MP),
    )

    return jax.shard_map(
        per_device,
        mesh=split,
        in_specs=placed,
        out_specs=(
            P(),
            P(None, DP),
            P(None, DP),
            P(DP, MP),
            P(DP, MP),
            P(DP, MP),
            P(MP, DP),
            P(DP, MP),
        ),
        check_vma=False,
    )
```

```python
import math

import jax
import jax.numpy as jnp
import numpy as np
from jax import lax
from jax.experimental import pallas as pl
from jax.experimental.pallas import tpu as pltpu
from jax.sharding import Mesh
from jax.sharding import PartitionSpec as P


WIDTH = 1280
PATCH = 32
PATCHES = 16
HEAD_DIM = 80
CHANNELS = 10
BLOCKS = 64
OWN = WIDTH // BLOCKS
TOKENS = 128
COLS = 320
WIDE = 384
BASIS = PATCH + PATCHES
TILES = (BASIS // 8) * (3 * WIDE // 128)
DP = ("dp_0", "dp_1", "dp_2")
XY = ("dp_0", "dp_2")
Z = "dp_1"
GROUPS = 16
DEPTH = 4
GROUP_ROWS = DEPTH * OWN
SMALL = 8 * BLOCKS // GROUPS
LINED = 32
PACKED = 5 * GROUP_ROWS // 2
GAIN_LANE = COLS + PATCH + PATCHES
FIRST = [(0, 1), (1, 0), (2, 3), (3, 2)]
SECOND = [(0, 3), (3, 0), (1, 2), (2, 1)]
FOURTH = [(0, 2), (2, 0), (1, 3), (3, 1)]
HALF = WIDTH // 2
MP = ("mp_0", "mp_1")
HEADS = [slice(at, at + HEAD_DIM) for at in range(0, COLS, HEAD_DIM)]
EPS = 1e-06
STAT_EPS = 1e-05
RADIUS = 0.05
SCALE = 1.0 / math.sqrt(HEAD_DIM)
GRANT = 16 * 1024 * 1024
BF = jnp.bfloat16
F32 = jnp.float32


def nn(a, b):
    return lax.dot_general(a, b, (((1,), (0,)), ((), ())), preferred_element_type=F32)


def nt(a, b):
    return lax.dot_general(a, b, (((1,), (1,)), ((), ())), preferred_element_type=F32)


def tn(a, b):
    return lax.dot_general(a, b, (((0,), (0,)), ((), ())), preferred_element_type=F32)


def two(x):
    high = x.astype(BF)
    return high, (x - high.astype(F32)).astype(BF)


def position_table():
    half = WIDTH // 2
    freqs = np.exp(np.float32(-math.log(10000.0)) * np.arange(half, dtype=np.float32) / np.float32(half))
    angles = np.arange(PATCHES, dtype=np.float32)[:, None] * freqs[None, :]
    table = np.concatenate([np.sin(angles), np.cos(angles)], axis=1).astype(np.float32)
    return np.ascontiguousarray(table.reshape(PATCHES, BLOCKS, OWN).transpose(1, 0, 2))


def turned_table():
    table = position_table().transpose(0, 2, 1)
    high = table.astype(jnp.bfloat16)
    low = (table - high.astype(np.float32)).astype(jnp.bfloat16)
    return np.concatenate([high, low], axis=2)


def call(body, outs, *args, grant=GRANT, far=(), scratch=()):
    spaces = [pltpu.HBM if at in far else pltpu.VMEM for at in range(len(outs))]
    return pl.pallas_call(
        body,
        out_shape=[jax.ShapeDtypeStruct(s, d) for s, d in outs],
        **({"out_specs": [pl.BlockSpec(memory_space=space) for space in spaces]} if far else {}),
        scratch_shapes=scratch,
        compiler_params=pltpu.CompilerParams(vmem_limit_bytes=grant),
    )(*args)


def own_basis(embed_ref, table_ref):
    eye = lax.broadcasted_iota(jnp.int32, (PATCH, PATCH), 0) == lax.broadcasted_iota(jnp.int32, (PATCH, PATCH), 1)
    embed = nt(eye.astype(F32).astype(BF), embed_ref[...])
    return jnp.concatenate([embed, table_ref[lax.axis_index(DP)]], axis=0)


def basis_kernel(
    embed_ref, gains_ref, table_ref, turned_ref, wq_ref, wk_ref, wv_ref, exit_ref, head_ref, out_ref, block_ref
):
    high, low = two(own_basis(embed_ref, table_ref) * gains_ref[0:1, :].astype(F32))
    out_ref[...] = jnp.zeros_like(out_ref)
    for w, ref in enumerate((wq_ref, wk_ref, wv_ref)):
        weight = ref[...]
        part = nn(high, weight) + nn(low, weight)
        for i in range(BASIS // 8):
            rows = part[8 * i : 8 * i + 8]
            for j in range(3):
                at = 9 * i + 3 * w + j
                lanes = rows[:, 128 * j : min(128 * j + 128, COLS)]
                k, t = at // DEPTH, 8 * (at % DEPTH)
                out_ref[k, t : t + 8, 0 : lanes.shape[1]] = lanes
    second = lax.broadcasted_iota(jnp.int32, (2, 1), 0).astype(F32).astype(BF)
    block_ref[...] = jnp.zeros_like(block_ref)
    block_ref[0:OWN, 0:COLS] = exit_ref[...]
    block_ref[0:OWN, COLS : COLS + PATCH] = embed_ref[...]
    block_ref[0:OWN, COLS + PATCH : WIDE] = turned_ref[lax.axis_index(DP)]
    block_ref[0:OWN, GAIN_LANE : GAIN_LANE + 1] = tn(gains_ref[...], second).astype(BF)
    block_ref[LINED : LINED + OWN, 0:COLS] = head_ref[...]


def from_tiles(ref):
    def tile(at):
        return ref[at // DEPTH, 8 * (at % DEPTH) : 8 * (at % DEPTH) + 8, :]

    return jnp.concatenate(
        [jnp.concatenate([tile(9 * i + j) for j in range(9)], axis=1) for i in range(BASIS // 8)], axis=0
    )


def blocks(ref, lanes=slice(0, WIDE)):
    rows = ref[:, :, lanes]
    return rows.reshape(WIDTH, rows.shape[2])


def spread_halves(value, mine_ref, other_ref):
    north = lax.axis_index("mp_1") == 1
    mine_ref[...] = jnp.where(north, value[HALF:], value[:HALF]).astype(BF)
    other_ref[...] = jnp.where(north, value[:HALF], value[HALF:]).astype(BF)


def joined_halves(mine_ref, other_ref):
    north = lax.axis_index("mp_1") == 1
    mine, other = mine_ref[...].astype(F32), other_ref[...].astype(F32)
    return jnp.concatenate([jnp.where(north, other, mine), jnp.where(north, mine, other)], axis=0)


def raw_projections(tiles_ref, basis):
    high, low = two(from_tiles(tiles_ref))
    return tn(jnp.concatenate([high, low], axis=0), jnp.concatenate([basis, basis], axis=0))


def first_residual(exit_ref, basis_ref):
    lanes = blocks(exit_ref, slice(256, 384))
    entries = basis_ref[...]
    return nn(lanes, jnp.concatenate([jnp.zeros_like(entries), entries], axis=0))


def causal_mask():
    j = lax.broadcasted_iota(jnp.int32, (TOKENS, TOKENS), 0)
    i = lax.broadcasted_iota(jnp.int32, (TOKENS, TOKENS), 1)
    same = lax.shift_right_logical(j, 4) == lax.shift_right_logical(i, 4)
    return same & (j <= i)


def attention(exit_ref, tiles_ref, basis_ref):
    residual = first_residual(exit_ref, basis_ref)
    factor = lax.rsqrt(jnp.sum(residual * residual, axis=0, keepdims=True) / WIDTH + EPS)
    raw = raw_projections(tiles_ref, basis_ref[0:BASIS, :])
    queries, keys, values = ((raw[w * WIDE : w * WIDE + COLS] * factor).astype(BF) for w in range(3))
    mask = causal_mask()
    all_probs, context = [], []
    for at in HEADS:
        scores = tn(keys[at], queries[at]) * SCALE
        raised = jnp.where(mask, jnp.exp(scores), 0.0)
        probs = raised / jnp.sum(raised, axis=0, keepdims=True)
        all_probs.append(probs)
        context.append(nn(values[at], probs.astype(BF)).astype(BF))
    return factor, raw, queries, keys, values, all_probs, context


def attention_kernel(exit_ref, tiles_ref, basis_ref, mine_ref, other_ref):
    context = attention(exit_ref, tiles_ref, basis_ref)[-1]
    context = jnp.concatenate([*context, jnp.zeros((WIDE - COLS, TOKENS), BF)], axis=0)
    spread_halves(nn(blocks(exit_ref), context), mine_ref, other_ref)


def gain_column(exit_ref):
    return blocks(exit_ref, slice(256, 384))[:, GAIN_LANE - 256 : GAIN_LANE - 255].astype(F32)


def lower_upper(x):
    grouped = x.reshape(GROUPS, GROUP_ROWS, TOKENS)
    half = GROUP_ROWS // 2
    return [part.reshape(WIDTH // 2, TOKENS) for part in (grouped[:, :half], grouped[:, half:])]


def head_kernel(
    exit_ref,
    head_ref,
    basis_ref,
    half_ref,
    rest_ref,
    target_ref,
    mine_ref,
    other_ref,
    grad_out_ref,
    residual_out_ref,
    grad_ref,
    residual_ref,
    grad_sem,
    residual_sem,
):
    residual = first_residual(exit_ref, basis_ref) + joined_halves(half_ref, rest_ref)
    residual_ref[0:WIDTH, :] = residual
    factor = lax.rsqrt(jnp.sum(residual * residual, axis=0, keepdims=True) / WIDTH + EPS)
    scaled = residual * factor * gain_column(exit_ref)
    normed = scaled.astype(BF)
    low, high = (part.astype(BF) for part in lower_upper(scaled))
    wide = jnp.concatenate(
        [head_ref[:, GROUP_ROWS * at : GROUP_ROWS * (at + 1), :].reshape(WIDTH, 128) for at in range(2)], axis=1
    )
    narrow = head_ref[:, 2 * GROUP_ROWS :, :].reshape(WIDTH // 2, 128)
    forecast = jnp.concatenate([tn(wide, normed), tn(narrow, low)[0:64] + tn(narrow, high)[64:128]], axis=0)
    column = lax.broadcasted_iota(jnp.int32, (COLS, 1), 0).astype(F32)
    step = jnp.floor((column + 0.5) * 0.1)
    channel = column - CHANNELS * step
    spread = (step == lax.broadcasted_iota(jnp.int32, (COLS, PATCH), 1).astype(F32)).astype(F32).astype(BF)
    target = target_ref[...]
    first, rest = target.astype(BF), target
    rest = rest - first.astype(F32)
    second, third = two(rest)
    expanded = nn(spread, first) + (nn(spread, second) + nn(spread, third))
    error = expanded - forecast
    share = channel / CHANNELS
    mean_channel = channel == 0.0
    inside = error / -RADIUS
    tail = jnp.exp(-jnp.abs(inside))
    softplus = jnp.maximum(inside, 0.0) + jnp.log1p(tail)
    sigmoid = jnp.where(inside >= 0.0, 1.0, tail) / (1.0 + tail)
    terms = jnp.where(mean_channel, error * error, share * error + RADIUS * softplus)
    residual_ref[WIDTH:, :] = jnp.broadcast_to(jnp.sum(terms, axis=0, keepdims=True), (8, TOKENS))
    residual_copy = pltpu.make_async_copy(residual_ref, residual_out_ref, residual_sem)
    residual_copy.start()
    slope = (jnp.where(mean_channel, -2.0 * error, sigmoid - share) * (1.0 / 128.0)).astype(BF)
    blank = jnp.zeros((64, TOKENS), BF)
    below = jnp.concatenate([slope[256:], blank], axis=0)
    above = jnp.concatenate([blank, slope[256:]], axis=0)
    grad = nt(normed, slope[0:256]).astype(BF)
    for at in range(2):
        grad_ref[:, GROUP_ROWS * at : GROUP_ROWS * (at + 1), :] = grad[:, 128 * at : 128 * at + 128].reshape(
            GROUPS, GROUP_ROWS, 128
        )
    grad = nt(low, below) + nt(high, above)
    grad_ref[:, 2 * GROUP_ROWS :, :] = grad.reshape(GROUPS, GROUP_ROWS // 2, 128).astype(BF)
    grad_copy = pltpu.make_async_copy(grad_ref, grad_out_ref, grad_sem)
    grad_copy.start()
    ends = [nn(narrow, part).reshape(GROUPS, GROUP_ROWS // 2, TOKENS) for part in (below, above)]
    back = nn(wide, slope[0:256]) + jnp.concatenate(ends, axis=1).reshape(WIDTH, TOKENS)
    spread_halves(back, mine_ref, other_ref)
    residual_copy.wait()
    grad_copy.wait()


def backward_kernel(
    exit_ref,
    tiles_ref,
    basis_ref,
    half_ref,
    rest_ref,
    residual_ref,
    grad_out_ref,
    out_ref,
    grad_ref,
    grad_sem,
):
    factor_zero, raw, queries, keys, values, all_probs, context = attention(exit_ref, tiles_ref, basis_ref)
    basis = basis_ref[0:BASIS, :]
    patches = basis_ref[0:PATCH, :]
    upstream = joined_halves(half_ref, rest_ref)
    residual = residual_ref[0:WIDTH, :]
    factor = lax.rsqrt(jnp.sum(residual * residual, axis=0, keepdims=True) / WIDTH + EPS)
    weighted = gain_column(exit_ref) * upstream
    inner = jnp.sum(weighted * residual, axis=0, keepdims=True) / WIDTH
    low = (factor * weighted - residual * (factor * factor * factor * inner)).astype(BF)
    grad = nt(low, jnp.concatenate([*context, patches, jnp.zeros_like(patches)], axis=0))
    lane = lax.broadcasted_iota(jnp.int32, (1, WIDE), 1)
    gain_high, gain_low = two(jnp.sum(upstream * residual * factor, axis=1, keepdims=True))
    grad = jnp.where(lane == COLS + PATCH, gain_high.astype(F32), grad)
    grad = jnp.where(lane == COLS + PATCH + 1, gain_low.astype(F32), grad)
    grad_ref[...] = grad.astype(BF).reshape(GROUPS, GROUP_ROWS, WIDE)
    grad_copy = pltpu.make_async_copy(grad_ref, grad_out_ref, grad_sem)
    grad_copy.start()
    context_grad = tn(blocks(exit_ref), low)[0:COLS].astype(BF)
    backs = ([], [], [])
    for at, probs in zip(HEADS, all_probs):
        slope = context_grad[at]
        prob_grad = tn(values[at], slope)
        value_back = nt(slope, probs.astype(BF))
        centred = prob_grad - jnp.sum(probs * prob_grad, axis=0, keepdims=True)
        score_grad = (probs * centred * SCALE).astype(BF)
        backs[0].append(nn(keys[at], score_grad).astype(BF))
        backs[1].append(nt(queries[at], score_grad).astype(BF))
        backs[2].append(value_back.astype(BF))
    gap = jnp.zeros((WIDE - COLS, TOKENS), BF)
    back = jnp.concatenate([*backs[0], gap, *backs[1], gap, *backs[2], gap], axis=0)
    factor = factor_zero
    entries = basis.astype(F32)
    high, low = two(entries * factor)
    total = nt(high, back) + nt(low, back)
    inner = jnp.sum(back.astype(F32) * raw, axis=0, keepdims=True) / WIDTH
    high, low = two(entries * (factor * factor * factor * inner))
    mixed = nt(high, patches) + nt(low, patches)
    blank = jnp.zeros((8, 128 - PATCH), F32)
    tiles = [total[8 * i : 8 * i + 8, 128 * j : 128 * j + 128] for i in range(BASIS // 8) for j in range(9)]
    tiles += [jnp.concatenate([mixed[8 * i : 8 * i + 8], blank], axis=1) for i in range(BASIS // 8)]
    tiles += [residual_ref[WIDTH:, :]]
    tiles += [jnp.zeros((8, 128), F32)] * (BLOCKS - len(tiles))
    for k in range(GROUPS):
        out_ref[k] = jnp.concatenate(tiles[DEPTH * k : DEPTH * k + DEPTH], axis=0)
    grad_copy.wait()


def group_sum(ref):
    total = ref[0].astype(F32)
    for k in range(1, GROUPS):
        total += ref[k].astype(F32)
    return total


def gather_kernel(tiles_ref, own_ref, first_ref, second_ref, fourth_ref, total_ref, exit_ref, head_ref):
    total_ref[...] = group_sum(tiles_ref)
    parts = [ref[...].astype(F32) for ref in (own_ref, first_ref, second_ref, fourth_ref)]
    exits = jnp.concatenate([p[0:OWN] for p in parts], axis=0).astype(BF)
    heads = jnp.concatenate([p[LINED : LINED + OWN] for p in parts], axis=0)
    half = GROUP_ROWS // 2
    narrow = jnp.concatenate([heads[:half, 256:320], heads[half:, 256:320]], axis=1)
    heads = jnp.concatenate([heads[:, 0:128], heads[:, 128:256], narrow], axis=0).astype(BF)
    for k in range(GROUPS):
        exit_ref[k] = exits
        head_ref[k] = heads


def total_kernel(one_ref, other_ref, out_ref):
    total = one_ref[...] + other_ref[...]
    for k in range(GROUPS):
        out_ref[k] = total


def scatter_kernel(exit_ref, head_ref, keep_ref, send_ref):
    exits, heads = group_sum(exit_ref), group_sum(head_ref)
    narrow = heads[2 * GROUP_ROWS :]
    narrow = jnp.concatenate([narrow, jnp.concatenate([narrow[:, 64:], narrow[:, :64]], axis=1)], axis=0)
    heads = jnp.concatenate([heads[:GROUP_ROWS], heads[GROUP_ROWS : 2 * GROUP_ROWS], narrow], axis=1)
    rows = [x[OWN * at : OWN * at + OWN] for at in range(DEPTH) for x in (exits, heads)]
    keep_ref[...] = jnp.concatenate(rows[:DEPTH], axis=0)
    send_ref[...] = jnp.concatenate(rows[DEPTH:], axis=0).astype(BF)


def exact(dims):
    def dot(a, b):
        return lax.dot_general(a, b, (dims, ((), ())), precision=lax.Precision.HIGHEST, preferred_element_type=F32)

    return dot


def last_kernel(
    tiles_ref,
    embed_ref,
    gains_ref,
    table_ref,
    wq_ref,
    wk_ref,
    wv_ref,
    q_ref,
    k_ref,
    v_ref,
    rest_ref,
):
    basis = own_basis(embed_ref, table_ref)
    total = from_tiles(tiles_ref)
    scaled_grad = exact(((0,), (0,)))(basis * gains_ref[0:1, :].astype(F32), total)
    plain_grad = exact(((0,), (0,)))(basis, total)
    embed = jnp.zeros((OWN, PATCH), F32)
    gain_zero = jnp.zeros((OWN, 1), F32)
    for w, (weight_ref, grad_ref) in enumerate(((wq_ref, q_ref), (wk_ref, k_ref), (wv_ref, v_ref))):
        weight = weight_ref[...].astype(F32)
        grad_ref[...] = scaled_grad[:, w * WIDE : w * WIDE + COLS]
        gain_zero += jnp.sum(weight * plain_grad[:, w * WIDE : w * WIDE + COLS], axis=1, keepdims=True)
        embed += exact(((1,), (1,)))(weight, total[0:PATCH, w * WIDE : w * WIDE + COLS])
    pick = (lax.broadcasted_iota(jnp.int32, (2, PATCH), 0) == 0).astype(F32)
    embed = embed * exact(((0,), (0,)))(gains_ref[...].astype(F32), pick)

    def small(at):
        return tiles_ref[at // DEPTH, 8 * (at % DEPTH) : 8 * (at % DEPTH) + 8, :]

    mixed = jnp.concatenate([small(TILES + i) for i in range(BASIS // 8)], axis=0)[:, 0:PATCH]
    embed = embed - exact(((0,), (0,)))(basis, mixed)
    rest_ref[...] = jnp.zeros_like(rest_ref)
    rest_ref[0:OWN, 0:PATCH] = embed
    rest_ref[0:OWN, PATCH : PATCH + 1] = gain_zero
    rest_ref[0:1, PATCH + 2 : PATCH + 3] = jnp.sum(small(TILES + BASIS // 8)[0:1, :], axis=1, keepdims=True)


def end_kernel(one_ref, other_ref, sums_ref, embed_ref, gains_ref, loss_ref, exit_grad_ref, head_grad_ref):
    exit_ref, head_ref = sums_ref[0:OWN, :], sums_ref[OWN : 2 * OWN, :]
    exit_grad_ref[...] = exit_ref[:, 0:COLS]
    head_grad_ref[...] = head_ref[:, 0:COLS]
    rest = one_ref[...] + other_ref[...]
    embed_ref[...] = rest[0:OWN, 0:PATCH] + exit_ref[:, COLS : COLS + PATCH]
    loss_ref[...] = rest[0:1, PATCH + 2 : PATCH + 3] / 1048576.0
    gain_one = exit_ref[:, COLS + PATCH : COLS + PATCH + 1] + exit_ref[:, COLS + PATCH + 1 : COLS + PATCH + 2]
    gain_one = jnp.concatenate([gain_one, jnp.zeros((24 - OWN, 1), F32)], axis=0)
    lane = lax.broadcasted_iota(jnp.int32, rest.shape, 1)
    gains_ref[...] = jnp.where(lane == PATCH + 1, gain_one, rest).T[PATCH : PATCH + 2, 0:OWN]


def swapped(x, axis):
    return lax.ppermute(x, axis, [(0, 1), (1, 0)])


def mp_sum(mine, other):
    half = (mine.astype(F32) + swapped(other, "mp_1").astype(F32)).astype(BF)
    half = (half.astype(F32) + swapped(half, "mp_0").astype(F32)).astype(BF)
    return half, swapped(half, "mp_1")


def over(x, axis):
    return lax.all_to_all(x, axis, 0, 0, tiled=True)


def along_z(x, pairs):
    return lax.ppermute(x, Z, pairs)


def z_total(x):
    x = x + along_z(x, FIRST)
    return call(total_kernel, [((GROUPS, SMALL, 128), F32)], x, along_z(x, SECOND))[0]


def after(x, *others):
    return lax.optimization_barrier((x, *others))[0]


def prepare(history, later):
    number = history.shape[0]
    centre = jnp.mean(history, axis=1, keepdims=True)
    spread = jnp.sqrt(jnp.mean((history - centre) * (history - centre), axis=1, keepdims=True) + STAT_EPS)
    normed = (history - centre) / spread
    ahead = (later - centre) / spread
    joined = jnp.concatenate([normed, ahead], axis=1).reshape(number, -1, PATCH)
    member = lax.axis_index(MP)
    target = lax.dynamic_slice_in_dim(joined, member + 1, PATCHES, 1).reshape(number * PATCHES, PATCH)
    patches = joined[:, :PATCHES].reshape(number * PATCHES, PATCH).astype(BF)
    return patches.T, target.T


def per_device(history, later, embed, gains, asking, lookup, content, attend_exit, outlook):
    table = jnp.asarray(position_table())
    embed_turned = embed.T
    tiles_like = ((GROUPS, SMALL, 128), F32)
    groups = ((GROUPS, GROUP_ROWS, WIDE), BF)
    tiles, block = call(
        basis_kernel,
        [tiles_like, ((2 * LINED, WIDE), BF)],
        embed_turned,
        gains,
        table,
        jnp.asarray(turned_table()),
        asking,
        lookup,
        content,
        attend_exit.T,
        outlook,
        grant=None,
    )
    tiles = over(tiles, XY)
    column = [along_z(block, pairs) for pairs in (FIRST, SECOND, FOURTH)]
    packed = ((GROUPS, PACKED, 128), BF)
    total, exit_all, head_all = call(
        gather_kernel, [((SMALL, 128), F32), groups, packed], tiles, block, *column
    )
    exit_all = over(exit_all, XY)
    tiles = z_total(total)

    patches, target = prepare(history, later)
    number = np.arange(TOKENS) % PATCHES
    place_hot = jnp.asarray((np.arange(PATCHES)[:, None] == number[None, :]), dtype=BF)
    low_hot = jnp.asarray((np.arange(PATCHES)[:, None] == number[None, :]) & (number[None, :] > 0), dtype=BF)
    basis = jnp.concatenate([patches, place_hot, low_hot], axis=0)
    tiles, exit_all, basis, target = lax.optimization_barrier((tiles, exit_all, basis, target))
    tiles = over(tiles, XY)
    head_all = over(after(head_all, tiles), XY)

    half = ((HALF, TOKENS), BF)
    mine, other = call(attention_kernel, [half, half], exit_all, tiles, basis)
    mine, other = mp_sum(mine, other)
    mine, other, head_grad, residual = call(
        head_kernel,
        [half, half, packed, ((WIDTH + 8, TOKENS), F32)],
        exit_all,
        head_all,
        basis,
        mine,
        other,
        target,
        far=(2, 3),
        scratch=[
            pltpu.VMEM(*packed),
            pltpu.VMEM((WIDTH + 8, TOKENS), F32),
            pltpu.SemaphoreType.DMA,
            pltpu.SemaphoreType.DMA,
        ],
    )
    head_grad = over(head_grad, XY)
    mine, other = mp_sum(mine, other)
    exit_grad, totals = call(
        backward_kernel,
        [groups, tiles_like],
        exit_all,
        tiles,
        basis,
        mine,
        other,
        residual,
        far=(0,),
        scratch=[pltpu.VMEM(*groups), pltpu.SemaphoreType.DMA],
    )
    totals = over(after(totals, head_grad), XY)
    exit_grad = over(after(exit_grad, totals), XY)
    totals = z_total(jnp.sum(totals, axis=0))
    totals = over(after(totals, exit_grad), XY)
    rows = (4 * OWN, WIDE)
    keep, send = call(scatter_kernel, [(rows, F32), (rows, BF)], exit_grad, head_grad)
    keep = keep + along_z(send, SECOND).astype(F32)
    sums = keep[: 2 * OWN] + along_z(keep[2 * OWN :].astype(BF), FIRST).astype(F32)
    own = ((OWN, COLS), F32)
    query_grad, key_grad, value_grad, rest = call(
        last_kernel,
        [own, own, own, ((24, 128), F32)],
        totals,
        embed_turned,
        gains,
        table,
        asking,
        lookup,
        content,
    )
    rest = rest + swapped(rest, "mp_1")
    embed_grad, gains_grad, loss_mean, output_grad, head_weight_grad = call(
        end_kernel,
        [((OWN, PATCH), F32), ((2, OWN), F32), ((1, 1), F32), own, own],
        rest,
        swapped(rest, "mp_0"),
        sums,
    )
    return (
        loss_mean[0, 0],
        embed_grad.T,
        gains_grad,
        query_grad,
        key_grad,
        value_grad,
        output_grad.T,
        head_weight_grad,
    )


def solution(mesh):
    split = Mesh(mesh.devices.reshape(4, 4, 4, 2, 2), ("dp_0", "dp_1", "dp_2", "mp_0", "mp_1"))
    placed = (
        P(DP, None),
        P(DP, None),
        P(None, DP),
        P(None, DP),
        P(DP, MP),
        P(DP, MP),
        P(DP, MP),
        P(MP, DP),
        P(DP, MP),
    )

    return jax.shard_map(
        per_device,
        mesh=split,
        in_specs=placed,
        out_specs=(
            P(),
            P(None, DP),
            P(None, DP),
            P(DP, MP),
            P(DP, MP),
            P(DP, MP),
            P(MP, DP),
            P(DP, MP),
        ),
        check_vma=False,
    )
```

```python
import math

import jax
import jax.numpy as jnp
import numpy as np
from jax import lax
from jax.experimental import pallas as pl
from jax.experimental.pallas import tpu as pltpu
from jax.sharding import Mesh
from jax.sharding import PartitionSpec as P


WIDTH = 1280
PATCH = 32
PATCHES = 16
HEAD_DIM = 80
CHANNELS = 10
BLOCKS = 64
OWN = WIDTH // BLOCKS
TOKENS = 128
COLS = 320
WIDE = 384
BASIS = PATCH + PATCHES
TILES = (BASIS // 8) * (3 * WIDE // 128)
DP = ("dp_0", "dp_1", "dp_2")
XY = ("dp_0", "dp_2")
Z = "dp_1"
GROUPS = 16
DEPTH = 4
GROUP_ROWS = DEPTH * OWN
SMALL = 8 * BLOCKS // GROUPS
LINED = 32
PACKED = 5 * GROUP_ROWS // 2
NEAR = 3 * OWN
SENT = 2 * SMALL + 3 * OWN + 4
GAIN_LANE = COLS + PATCH + PATCHES
FIRST = [(0, 1), (1, 0), (2, 3), (3, 2)]
SECOND = [(0, 3), (3, 0), (1, 2), (2, 1)]
FOURTH = [(0, 2), (2, 0), (1, 3), (3, 1)]
HALF = WIDTH // 2
MP = ("mp_0", "mp_1")
HEADS = [slice(at, at + HEAD_DIM) for at in range(0, COLS, HEAD_DIM)]
EPS = 1e-06
STAT_EPS = 1e-05
RADIUS = 0.05
SCALE = 1.0 / math.sqrt(HEAD_DIM)
GRANT = 16 * 1024 * 1024
BF = jnp.bfloat16
F32 = jnp.float32


def nn(a, b):
    return lax.dot_general(a, b, (((1,), (0,)), ((), ())), preferred_element_type=F32)


def nt(a, b):
    return lax.dot_general(a, b, (((1,), (1,)), ((), ())), preferred_element_type=F32)


def tn(a, b):
    return lax.dot_general(a, b, (((0,), (0,)), ((), ())), preferred_element_type=F32)


def two(x):
    high = x.astype(BF)
    return high, (x - high.astype(F32)).astype(BF)


def position_table():
    half = WIDTH // 2
    freqs = np.exp(np.float32(-math.log(10000.0)) * np.arange(half, dtype=np.float32) / np.float32(half))
    angles = np.arange(PATCHES, dtype=np.float32)[:, None] * freqs[None, :]
    table = np.concatenate([np.sin(angles), np.cos(angles)], axis=1).astype(np.float32)
    return np.ascontiguousarray(table.reshape(PATCHES, BLOCKS, OWN).transpose(1, 0, 2))


def turned_table():
    table = position_table().transpose(0, 2, 1)
    high = table.astype(jnp.bfloat16)
    low = (table - high.astype(np.float32)).astype(jnp.bfloat16)
    return np.concatenate([high, low], axis=2)


def call(body, outs, *args, grant=GRANT, far=(), scratch=()):
    spaces = [pltpu.HBM if at in far else pltpu.VMEM for at in range(len(outs))]
    return pl.pallas_call(
        body,
        out_shape=[jax.ShapeDtypeStruct(s, d) for s, d in outs],
        **({"out_specs": [pl.BlockSpec(memory_space=space) for space in spaces]} if far else {}),
        scratch_shapes=scratch,
        compiler_params=pltpu.CompilerParams(vmem_limit_bytes=grant),
    )(*args)


def own_basis(embed_ref, table_ref):
    eye = lax.broadcasted_iota(jnp.int32, (PATCH, PATCH), 0) == lax.broadcasted_iota(jnp.int32, (PATCH, PATCH), 1)
    embed = nt(eye.astype(F32).astype(BF), embed_ref[...])
    return jnp.concatenate([embed, table_ref[lax.axis_index(DP)]], axis=0)


def basis_kernel(
    embed_ref, gains_ref, table_ref, turned_ref, wq_ref, wk_ref, wv_ref, exit_ref, head_ref, out_ref, block_ref
):
    high, low = two(own_basis(embed_ref, table_ref) * gains_ref[0:1, :].astype(F32))
    out_ref[...] = jnp.zeros_like(out_ref)
    for w, ref in enumerate((wq_ref, wk_ref, wv_ref)):
        weight = ref[...]
        part = nn(high, weight) + nn(low, weight)
        for i in range(BASIS // 8):
            rows = part[8 * i : 8 * i + 8]
            for j in range(3):
                at = 9 * i + 3 * w + j
                lanes = rows[:, 128 * j : min(128 * j + 128, COLS)]
                k, t = at // DEPTH, 8 * (at % DEPTH)
                out_ref[k, t : t + 8, 0 : lanes.shape[1]] = lanes
    second = lax.broadcasted_iota(jnp.int32, (2, 1), 0).astype(F32).astype(BF)
    block_ref[...] = jnp.zeros_like(block_ref)
    block_ref[0:OWN, 0:COLS] = exit_ref[...]
    block_ref[0:OWN, COLS : COLS + PATCH] = embed_ref[...]
    block_ref[0:OWN, COLS + PATCH : WIDE] = turned_ref[lax.axis_index(DP)]
    block_ref[0:OWN, GAIN_LANE : GAIN_LANE + 1] = tn(gains_ref[...], second).astype(BF)
    block_ref[LINED : LINED + OWN, 0:COLS] = head_ref[...]


def from_tiles(ref):
    def tile(at):
        return ref[at // DEPTH, 8 * (at % DEPTH) : 8 * (at % DEPTH) + 8, :]

    return jnp.concatenate(
        [jnp.concatenate([tile(9 * i + j) for j in range(9)], axis=1) for i in range(BASIS // 8)], axis=0
    )


def blocks(ref, lanes=slice(0, WIDE)):
    rows = ref[:, :, lanes]
    return rows.reshape(WIDTH, rows.shape[2])


def spread_halves(value, mine_ref, other_ref):
    north = lax.axis_index("mp_1") == 1
    mine_ref[...] = jnp.where(north, value[HALF:], value[:HALF]).astype(BF)
    other_ref[...] = jnp.where(north, value[:HALF], value[HALF:]).astype(BF)


def joined_halves(mine_ref, other_ref):
    north = lax.axis_index("mp_1") == 1
    mine, other = mine_ref[...].astype(F32), other_ref[...].astype(F32)
    return jnp.concatenate([jnp.where(north, other, mine), jnp.where(north, mine, other)], axis=0)


def both_from(ref):
    def tile(at, side):
        rows = ref[at // DEPTH, side * SMALL : (side + 1) * SMALL, :].astype(F32)
        return rows[8 * (at % DEPTH) : 8 * (at % DEPTH) + 8]

    return [
        jnp.concatenate(
            [jnp.concatenate([tile(9 * i + j, side) for j in range(9)], axis=1) for i in range(BASIS // 8)], axis=0
        ).astype(BF)
        for side in range(2)
    ]


def raw_projections(tiles_ref, basis):
    high, low = both_from(tiles_ref)
    return tn(jnp.concatenate([high, low], axis=0), jnp.concatenate([basis, basis], axis=0))


def first_residual(exit_ref, basis_ref):
    lanes = blocks(exit_ref, slice(256, 384))
    entries = basis_ref[...]
    return nn(lanes, jnp.concatenate([jnp.zeros_like(entries), entries], axis=0))


def causal_mask():
    j = lax.broadcasted_iota(jnp.int32, (TOKENS, TOKENS), 0)
    i = lax.broadcasted_iota(jnp.int32, (TOKENS, TOKENS), 1)
    same = lax.shift_right_logical(j, 4) == lax.shift_right_logical(i, 4)
    return same & (j <= i)


def attention(exit_ref, tiles_ref, basis_ref):
    residual = first_residual(exit_ref, basis_ref)
    factor = lax.rsqrt(jnp.sum(residual * residual, axis=0, keepdims=True) / WIDTH + EPS)
    raw = raw_projections(tiles_ref, basis_ref[0:BASIS, :])
    queries, keys, values = ((raw[w * WIDE : w * WIDE + COLS] * factor).astype(BF) for w in range(3))
    mask = causal_mask()
    all_probs, context = [], []
    for at in HEADS:
        scores = tn(keys[at], queries[at]) * SCALE
        raised = jnp.where(mask, jnp.exp(scores), 0.0)
        probs = raised / jnp.sum(raised, axis=0, keepdims=True)
        all_probs.append(probs)
        context.append(nn(values[at], probs.astype(BF)).astype(BF))
    return factor, raw, queries, keys, values, all_probs, context


def attention_kernel(
    near_ref, tiles_ref, basis_ref, mine_ref, other_ref, exit_ref
):
    for k in range(GROUPS):
        fourth = tiles_ref[k, 2 * SMALL :, :].astype(F32)
        lanes = [fourth[OWN * j : OWN * j + OWN] for j in range(3)]
        rows = jnp.concatenate([near_ref[k].astype(F32), jnp.concatenate(lanes, axis=1)], axis=0)
        exit_ref[k] = rows.astype(BF)
    context = attention(exit_ref, tiles_ref, basis_ref)[-1]
    context = jnp.concatenate([*context, jnp.zeros((WIDE - COLS, TOKENS), BF)], axis=0)
    spread_halves(nn(blocks(exit_ref), context), mine_ref, other_ref)


def gain_column(exit_ref):
    return blocks(exit_ref, slice(256, 384))[:, GAIN_LANE - 256 : GAIN_LANE - 255].astype(F32)


def lower_upper(x):
    grouped = x.reshape(GROUPS, GROUP_ROWS, TOKENS)
    half = GROUP_ROWS // 2
    return [part.reshape(WIDTH // 2, TOKENS) for part in (grouped[:, :half], grouped[:, half:])]


def head_kernel(
    exit_ref,
    head_ref,
    basis_ref,
    half_ref,
    rest_ref,
    target_ref,
    mine_ref,
    other_ref,
    grad_out_ref,
    residual_out_ref,
    grad_ref,
    residual_ref,
    grad_sem,
    residual_sem,
):
    residual = first_residual(exit_ref, basis_ref) + joined_halves(half_ref, rest_ref)
    residual_ref[0:WIDTH, :] = residual
    factor = lax.rsqrt(jnp.sum(residual * residual, axis=0, keepdims=True) / WIDTH + EPS)
    scaled = residual * factor * gain_column(exit_ref)
    normed = scaled.astype(BF)
    low, high = (part.astype(BF) for part in lower_upper(scaled))
    wide = jnp.concatenate(
        [head_ref[:, GROUP_ROWS * at : GROUP_ROWS * (at + 1), :].reshape(WIDTH, 128) for at in range(2)], axis=1
    )
    narrow = head_ref[:, 2 * GROUP_ROWS :, :].reshape(WIDTH // 2, 128)
    forecast = jnp.concatenate([tn(wide, normed), tn(narrow, low)[0:64] + tn(narrow, high)[64:128]], axis=0)
    column = lax.broadcasted_iota(jnp.int32, (COLS, 1), 0).astype(F32)
    step = jnp.floor((column + 0.5) * 0.1)
    channel = column - CHANNELS * step
    spread = (step == lax.broadcasted_iota(jnp.int32, (COLS, PATCH), 1).astype(F32)).astype(F32).astype(BF)
    target = target_ref[...]
    first, rest = target.astype(BF), target
    rest = rest - first.astype(F32)
    second, third = two(rest)
    expanded = nn(spread, first) + (nn(spread, second) + nn(spread, third))
    error = expanded - forecast
    share = channel / CHANNELS
    mean_channel = channel == 0.0
    inside = error / -RADIUS
    tail = jnp.exp(-jnp.abs(inside))
    softplus = jnp.maximum(inside, 0.0) + jnp.log1p(tail)
    sigmoid = jnp.where(inside >= 0.0, 1.0, tail) / (1.0 + tail)
    terms = jnp.where(mean_channel, error * error, share * error + RADIUS * softplus)
    residual_ref[WIDTH:, :] = jnp.broadcast_to(jnp.sum(terms, axis=0, keepdims=True), (8, TOKENS))
    residual_copy = pltpu.make_async_copy(residual_ref, residual_out_ref, residual_sem)
    residual_copy.start()
    slope = (jnp.where(mean_channel, -2.0 * error, sigmoid - share) * (1.0 / 128.0)).astype(BF)
    blank = jnp.zeros((64, TOKENS), BF)
    below = jnp.concatenate([slope[256:], blank], axis=0)
    above = jnp.concatenate([blank, slope[256:]], axis=0)
    grad = nt(normed, slope[0:256]).astype(BF)
    for at in range(2):
        grad_ref[:, GROUP_ROWS * at : GROUP_ROWS * (at + 1), :] = grad[:, 128 * at : 128 * at + 128].reshape(
            GROUPS, GROUP_ROWS, 128
        )
    grad = nt(low, below) + nt(high, above)
    grad_ref[:, 2 * GROUP_ROWS :, :] = grad.reshape(GROUPS, GROUP_ROWS // 2, 128).astype(BF)
    grad_copy = pltpu.make_async_copy(grad_ref, grad_out_ref, grad_sem)
    grad_copy.start()
    ends = [nn(narrow, part).reshape(GROUPS, GROUP_ROWS // 2, TOKENS) for part in (below, above)]
    back = nn(wide, slope[0:256]) + jnp.concatenate(ends, axis=1).reshape(WIDTH, TOKENS)
    spread_halves(back, mine_ref, other_ref)
    residual_copy.wait()
    grad_copy.wait()


def backward_kernel(
    exit_ref,
    tiles_ref,
    basis_ref,
    half_ref,
    rest_ref,
    residual_ref,
    grad_out_ref,
    out_ref,
    grad_ref,
    grad_sem,
):
    factor_zero, raw, queries, keys, values, all_probs, context = attention(exit_ref, tiles_ref, basis_ref)
    basis = basis_ref[0:BASIS, :]
    patches = basis_ref[0:PATCH, :]
    upstream = joined_halves(half_ref, rest_ref)
    residual = residual_ref[0:WIDTH, :]
    factor = lax.rsqrt(jnp.sum(residual * residual, axis=0, keepdims=True) / WIDTH + EPS)
    weighted = gain_column(exit_ref) * upstream
    inner = jnp.sum(weighted * residual, axis=0, keepdims=True) / WIDTH
    low = (factor * weighted - residual * (factor * factor * factor * inner)).astype(BF)
    grad = nt(low, jnp.concatenate([*context, patches, jnp.zeros_like(patches)], axis=0))
    lane = lax.broadcasted_iota(jnp.int32, (1, WIDE), 1)
    gain_high, gain_low = two(jnp.sum(upstream * residual * factor, axis=1, keepdims=True))
    grad = jnp.where(lane == COLS + PATCH, gain_high.astype(F32), grad)
    grad = jnp.where(lane == COLS + PATCH + 1, gain_low.astype(F32), grad)
    grad_ref[...] = grad.astype(BF).reshape(GROUPS, GROUP_ROWS, WIDE)
    grad_copy = pltpu.make_async_copy(grad_ref, grad_out_ref, grad_sem)
    grad_copy.start()
    context_grad = tn(blocks(exit_ref), low)[0:COLS].astype(BF)
    backs = ([], [], [])
    for at, probs in zip(HEADS, all_probs):
        slope = context_grad[at]
        prob_grad = tn(values[at], slope)
        value_back = nt(slope, probs.astype(BF))
        centred = prob_grad - jnp.sum(probs * prob_grad, axis=0, keepdims=True)
        score_grad = (probs * centred * SCALE).astype(BF)
        backs[0].append(nn(keys[at], score_grad).astype(BF))
        backs[1].append(nt(queries[at], score_grad).astype(BF))
        backs[2].append(value_back.astype(BF))
    gap = jnp.zeros((WIDE - COLS, TOKENS), BF)
    back = jnp.concatenate([*backs[0], gap, *backs[1], gap, *backs[2], gap], axis=0)
    factor = factor_zero
    entries = basis.astype(F32)
    high, low = two(entries * factor)
    total = nt(high, back) + nt(low, back)
    inner = jnp.sum(back.astype(F32) * raw, axis=0, keepdims=True) / WIDTH
    high, low = two(entries * (factor * factor * factor * inner))
    mixed = nt(high, patches) + nt(low, patches)
    blank = jnp.zeros((8, 128 - PATCH), F32)
    tiles = [total[8 * i : 8 * i + 8, 128 * j : 128 * j + 128] for i in range(BASIS // 8) for j in range(9)]
    tiles += [jnp.concatenate([mixed[8 * i : 8 * i + 8], blank], axis=1) for i in range(BASIS // 8)]
    tiles += [residual_ref[WIDTH:, :]]
    tiles += [jnp.zeros((8, 128), F32)] * (BLOCKS - len(tiles))
    for k in range(GROUPS):
        out_ref[k] = jnp.concatenate(tiles[DEPTH * k : DEPTH * k + DEPTH], axis=0)
    grad_copy.wait()


def group_sum(ref):
    total = ref[0].astype(F32)
    for k in range(1, GROUPS):
        total += ref[k].astype(F32)
    return total


def gather_kernel(tiles_ref, own_ref, first_ref, second_ref, total_ref, exit_ref):
    total_ref[...] = group_sum(tiles_ref)
    parts = [ref[0:OWN, :].astype(F32) for ref in (own_ref, first_ref, second_ref)]
    exits = jnp.concatenate(parts, axis=0).astype(BF)
    for k in range(GROUPS):
        exit_ref[k] = exits


def merged_kernel(one_ref, other_ref, fourth_ref, out_ref):
    high, low = two(one_ref[...] + other_ref[...])
    block = fourth_ref[0:OWN, :].astype(F32)
    lanes = [block[:, 128 * j : 128 * j + 128] for j in range(3)]
    parts = [high.astype(F32), low.astype(F32), *lanes, jnp.zeros((4, 128), F32)]
    rows = jnp.concatenate(parts, axis=0).astype(BF)
    for k in range(GROUPS):
        out_ref[k] = rows


def pack_kernel(own_ref, first_ref, second_ref, fourth_ref, head_ref):
    heads = jnp.concatenate(
        [ref[LINED : LINED + OWN, :].astype(F32) for ref in (own_ref, first_ref, second_ref, fourth_ref)], axis=0
    )
    half = GROUP_ROWS // 2
    narrow = jnp.concatenate([heads[:half, 256:320], heads[half:, 256:320]], axis=1)
    heads = jnp.concatenate([heads[:, 0:128], heads[:, 128:256], narrow], axis=0).astype(BF)
    for k in range(GROUPS):
        head_ref[k] = heads


def total_kernel(one_ref, other_ref, out_ref):
    total = one_ref[...] + other_ref[...]
    for k in range(GROUPS):
        out_ref[k] = total


def scatter_kernel(exit_ref, head_ref, keep_ref, send_ref):
    exits, heads = group_sum(exit_ref), group_sum(head_ref)
    narrow = heads[2 * GROUP_ROWS :]
    narrow = jnp.concatenate([narrow, jnp.concatenate([narrow[:, 64:], narrow[:, :64]], axis=1)], axis=0)
    heads = jnp.concatenate([heads[:GROUP_ROWS], heads[GROUP_ROWS : 2 * GROUP_ROWS], narrow], axis=1)
    rows = [x[OWN * at : OWN * at + OWN] for at in range(DEPTH) for x in (exits, heads)]
    keep_ref[...] = jnp.concatenate(rows[:DEPTH], axis=0)
    send_ref[...] = jnp.concatenate(rows[DEPTH:], axis=0).astype(BF)


def exact(dims):
    def dot(a, b):
        return lax.dot_general(a, b, (dims, ((), ())), precision=lax.Precision.HIGHEST, preferred_element_type=F32)

    return dot


def last_kernel(
    tiles_ref,
    embed_ref,
    gains_ref,
    table_ref,
    wq_ref,
    wk_ref,
    wv_ref,
    q_ref,
    k_ref,
    v_ref,
    rest_ref,
):
    basis = own_basis(embed_ref, table_ref)
    total = from_tiles(tiles_ref)
    scaled_grad = exact(((0,), (0,)))(basis * gains_ref[0:1, :].astype(F32), total)
    plain_grad = exact(((0,), (0,)))(basis, total)
    embed = jnp.zeros((OWN, PATCH), F32)
    gain_zero = jnp.zeros((OWN, 1), F32)
    for w, (weight_ref, grad_ref) in enumerate(((wq_ref, q_ref), (wk_ref, k_ref), (wv_ref, v_ref))):
        weight = weight_ref[...].astype(F32)
        grad_ref[...] = scaled_grad[:, w * WIDE : w * WIDE + COLS]
        gain_zero += jnp.sum(weight * plain_grad[:, w * WIDE : w * WIDE + COLS], axis=1, keepdims=True)
        embed += exact(((1,), (1,)))(weight, total[0:PATCH, w * WIDE : w * WIDE + COLS])
    pick = (lax.broadcasted_iota(jnp.int32, (2, PATCH), 0) == 0).astype(F32)
    embed = embed * exact(((0,), (0,)))(gains_ref[...].astype(F32), pick)

    def small(at):
        return tiles_ref[at // DEPTH, 8 * (at % DEPTH) : 8 * (at % DEPTH) + 8, :]

    mixed = jnp.concatenate([small(TILES + i) for i in range(BASIS // 8)], axis=0)[:, 0:PATCH]
    embed = embed - exact(((0,), (0,)))(basis, mixed)
    rest_ref[...] = jnp.zeros_like(rest_ref)
    rest_ref[0:OWN, 0:PATCH] = embed
    rest_ref[0:OWN, PATCH : PATCH + 1] = gain_zero
    rest_ref[0:1, PATCH + 2 : PATCH + 3] = jnp.sum(small(TILES + BASIS // 8)[0:1, :], axis=1, keepdims=True)


def end_kernel(one_ref, other_ref, sums_ref, embed_ref, gains_ref, loss_ref, exit_grad_ref, head_grad_ref):
    exit_ref, head_ref = sums_ref[0:OWN, :], sums_ref[OWN : 2 * OWN, :]
    exit_grad_ref[...] = exit_ref[:, 0:COLS]
    head_grad_ref[...] = head_ref[:, 0:COLS]
    rest = one_ref[...] + other_ref[...]
    embed_ref[...] = rest[0:OWN, 0:PATCH] + exit_ref[:, COLS : COLS + PATCH]
    loss_ref[...] = rest[0:1, PATCH + 2 : PATCH + 3] / 1048576.0
    gain_one = exit_ref[:, COLS + PATCH : COLS + PATCH + 1] + exit_ref[:, COLS + PATCH + 1 : COLS + PATCH + 2]
    gain_one = jnp.concatenate([gain_one, jnp.zeros((24 - OWN, 1), F32)], axis=0)
    lane = lax.broadcasted_iota(jnp.int32, rest.shape, 1)
    gains_ref[...] = jnp.where(lane == PATCH + 1, gain_one, rest).T[PATCH : PATCH + 2, 0:OWN]


def swapped(x, axis):
    return lax.ppermute(x, axis, [(0, 1), (1, 0)])


def mp_sum(mine, other):
    half = (mine.astype(F32) + swapped(other, "mp_1").astype(F32)).astype(BF)
    half = (half.astype(F32) + swapped(half, "mp_0").astype(F32)).astype(BF)
    return half, swapped(half, "mp_1")


def over(x, axis):
    return lax.all_to_all(x, axis, 0, 0, tiled=True)


def along_z(x, pairs):
    return lax.ppermute(x, Z, pairs)


def z_total(x):
    x = x + along_z(x, FIRST)
    return call(total_kernel, [((GROUPS, SMALL, 128), F32)], x, along_z(x, SECOND))[0]


def after(x, *others):
    return lax.optimization_barrier((x, *others))[0]


def prepare(history, later):
    number = history.shape[0]
    centre = jnp.mean(history, axis=1, keepdims=True)
    spread = jnp.sqrt(jnp.mean((history - centre) * (history - centre), axis=1, keepdims=True) + STAT_EPS)
    normed = (history - centre) / spread
    ahead = (later - centre) / spread
    joined = jnp.concatenate([normed, ahead], axis=1).reshape(number, -1, PATCH)
    member = lax.axis_index(MP)
    target = lax.dynamic_slice_in_dim(joined, member + 1, PATCHES, 1).reshape(number * PATCHES, PATCH)
    patches = joined[:, :PATCHES].reshape(number * PATCHES, PATCH).astype(BF)
    return patches.T, target.T


def per_device(history, later, embed, gains, asking, lookup, content, attend_exit, outlook):
    table = jnp.asarray(position_table())
    embed_turned = embed.T
    tiles_like = ((GROUPS, SMALL, 128), F32)
    groups = ((GROUPS, GROUP_ROWS, WIDE), BF)
    tiles, block = call(
        basis_kernel,
        [tiles_like, ((2 * LINED, WIDE), BF)],
        embed_turned,
        gains,
        table,
        jnp.asarray(turned_table()),
        asking,
        lookup,
        content,
        attend_exit.T,
        outlook,
        grant=None,
    )
    tiles = over(tiles, XY)
    arrived = []
    for pairs in (FIRST, SECOND, FOURTH):
        arrived.append(along_z(block, pairs))
    packed = ((GROUPS, PACKED, 128), BF)
    total, near_exit = call(
        gather_kernel, [((SMALL, 128), F32), ((GROUPS, NEAR, WIDE), BF)], tiles, block, *arrived[:2]
    )
    near_exit = over(near_exit, XY)
    total = total + along_z(total, FIRST)
    tiles = call(
        merged_kernel, [((GROUPS, SENT, 128), BF)], total, along_z(total, SECOND), arrived[2]
    )[0]
    head_all = call(pack_kernel, [packed], block, *arrived)[0]

    patches, target = prepare(history, later)
    number = np.arange(TOKENS) % PATCHES
    place_hot = jnp.asarray((np.arange(PATCHES)[:, None] == number[None, :]), dtype=BF)
    low_hot = jnp.asarray((np.arange(PATCHES)[:, None] == number[None, :]) & (number[None, :] > 0), dtype=BF)
    basis = jnp.concatenate([patches, place_hot, low_hot], axis=0)
    tiles, near_exit, basis, target = lax.optimization_barrier((tiles, near_exit, basis, target))
    tiles = over(tiles, XY)
    head_all = over(after(head_all, tiles), XY)

    half = ((HALF, TOKENS), BF)
    mine, other, exit_all = call(
        attention_kernel,
        [half, half, groups],
        near_exit,
        tiles,
        basis,
    )
    mine, other = mp_sum(mine, other)
    mine, other, head_grad, residual = call(
        head_kernel,
        [half, half, packed, ((WIDTH + 8, TOKENS), F32)],
        exit_all,
        head_all,
        basis,
        mine,
        other,
        target,
        far=(2, 3),
        scratch=[
            pltpu.VMEM(*packed),
            pltpu.VMEM((WIDTH + 8, TOKENS), F32),
            pltpu.SemaphoreType.DMA,
            pltpu.SemaphoreType.DMA,
        ],
    )
    head_grad = over(head_grad, XY)
    mine, other = mp_sum(mine, other)
    exit_grad, totals = call(
        backward_kernel,
        [groups, tiles_like],
        exit_all,
        tiles,
        basis,
        mine,
        other,
        residual,
        far=(0,),
        scratch=[pltpu.VMEM(*groups), pltpu.SemaphoreType.DMA],
    )
    totals = over(after(totals, head_grad), XY)
    exit_grad = over(after(exit_grad, totals), XY)
    totals = z_total(jnp.sum(totals, axis=0))
    totals = over(after(totals, exit_grad), XY)
    rows = (4 * OWN, WIDE)
    keep, send = call(scatter_kernel, [(rows, F32), (rows, BF)], exit_grad, head_grad)
    keep = keep + along_z(send, SECOND).astype(F32)
    sums = keep[: 2 * OWN] + along_z(keep[2 * OWN :].astype(BF), FIRST).astype(F32)
    own = ((OWN, COLS), F32)
    query_grad, key_grad, value_grad, rest = call(
        last_kernel,
        [own, own, own, ((24, 128), F32)],
        totals,
        embed_turned,
        gains,
        table,
        asking,
        lookup,
        content,
    )
    rest = rest + swapped(rest, "mp_1")
    embed_grad, gains_grad, loss_mean, output_grad, head_weight_grad = call(
        end_kernel,
        [((OWN, PATCH), F32), ((2, OWN), F32), ((1, 1), F32), own, own],
        rest,
        swapped(rest, "mp_0"),
        sums,
    )
    return (
        loss_mean[0, 0],
        embed_grad.T,
        gains_grad,
        query_grad,
        key_grad,
        value_grad,
        output_grad.T,
        head_weight_grad,
    )


def solution(mesh):
    split = Mesh(mesh.devices.reshape(4, 4, 4, 2, 2), ("dp_0", "dp_1", "dp_2", "mp_0", "mp_1"))
    placed = (
        P(DP, None),
        P(DP, None),
        P(None, DP),
        P(None, DP),
        P(DP, MP),
        P(DP, MP),
        P(DP, MP),
        P(MP, DP),
        P(DP, MP),
    )

    return jax.shard_map(
        per_device,
        mesh=split,
        in_specs=placed,
        out_specs=(
            P(),
            P(None, DP),
            P(None, DP),
            P(DP, MP),
            P(DP, MP),
            P(DP, MP),
            P(MP, DP),
            P(DP, MP),
        ),
        check_vma=False,
    )
```
